32 devices in a mesh: crop: 2 (over x), seq: 2 (over y), res: 8 (over z, core).
Axes of the slice: x: 2, y: 2, z: 4, core: 2. Of those that a mesh axis runs over, the one named last changes fastest.
Arguments:
- aligned_chain_embedding: bfloat16 [128, 32, 256], P(('crop', 'seq'), 'res'), parts along dimension 0, may hold values from -6 to 6
- alignment_mask: int32 [128, 32], P(('crop', 'seq'), 'res'), parts along dimension 0, may hold values from 0 to 1, as said below
- resolved_residue_mask: int32 [64], P('crop'), parts along dimension 0, may hold values 0 or 1
- pairwise_state: bfloat16 [64, 32, 128], P(('crop', 'seq'), 'res'), parts along dimension 0, may hold values from -8 to 8
- combined_projection_matrix: bfloat16 [256, 1024], replicated, may hold values from -0.375 to 0.375
- pair_bias_weight: bfloat16 [128, 8], replicated, may hold values from -8 to 8
- final_projection_matrix: bfloat16 [256, 256], replicated, may hold values from -0.375 to 0.375
- left_right_projection_matrix: bfloat16 [256, 64], replicated, may hold values from -1.5 to 1.5
- outer_mean_weight: bfloat16 [1024, 128], replicated, may hold values from -0.1875 to 0.1875
Outputs:
- alignment_output: bfloat16 [128, 32, 256], P(('crop', 'seq'), 'res'), parts along dimension 0
- pairwise_output: bfloat16 [64, 32, 128], P(('crop', 'seq'), 'res'), parts along dimension 0
The draws below stay inside these ranges and needn't reach their ends.
There are 2 independent parts, one for each index of `crop`. The reference program is written for one: setup_inputs(seed, part) draws one part's arguments, and reference() takes and returns one part's arrays. A program takes and returns all parts, laid end to end along the dimension named above; an argument that names none is the same for every part. Nothing has to cross between parts.
Inputs may be any that keep to these rules, and one draw needn't show every extreme that they name: `alignment_mask`: sequence 0 has no gaps.
All inputs are finite; a program needn't handle non-finite values.
Results may differ from the reference program's by a relative error of at most 0.013.
The reference program's roundings to bfloat16 on the way count: a program that leaves them out, or rounds other values in their place, can miss the bound.
Values may be sent and summed in bfloat16 or wider, within the bound.
A program may use at most 64 MiB of HBM per device.

```python
import math
import jax
import jax.numpy as jnp
from jax import lax

ROW_FEATURES = 256
CZ = 128
HEAD_NUMBER = 8
PER_HEAD_DIM = 32
PROJ_FEATURES = 32
ALIGNED_CHAINS = 64
WINDOW_AMINOS = 32


def draw_alignment_mask(key, part):
    permutation_indices = jnp.arange(ALIGNED_CHAINS, dtype=jnp.int32)[:, None]
    uniform_bound = 900 - 600 * permutation_indices // max(ALIGNED_CHAINS - 1, 1)
    random_token = jax.random.randint(key, (ALIGNED_CHAINS, WINDOW_AMINOS), 0, 1000, dtype=jnp.int32)
    keep = jnp.logical_or(random_token < uniform_bound, permutation_indices == 0)
    return keep.astype(jnp.int32)


def draw_pairwise_state(key, part):
    noise_key = jax.random.fold_in(key, 0)
    noise = jax.random.normal(noise_key, (WINDOW_AMINOS, WINDOW_AMINOS, CZ), jnp.float32)
    return jnp.clip(noise, -8.0, 8.0).astype(jnp.bfloat16)


def draw_pair_bias_weight(key, part):
    base_key = jax.random.fold_in(key, 0)
    weights = jax.random.normal(base_key, (CZ, HEAD_NUMBER), jnp.float32) / math.sqrt(CZ)
    return jnp.clip(weights, -8.0, 8.0).astype(jnp.bfloat16)


def set_ends(values, own_key, low, high):
    longest = values.shape.index(max(values.shape))
    spots = []
    for shift in (0, 1):
        where = [jax.random.randint(jax.random.fold_in(own_key, axis), (), 0, length) for axis, length in enumerate(values.shape)]
        where[longest] = (where[longest] + shift) % values.shape[longest]
        spots.append(tuple(where))
    return values.at[spots[0]].set(low).at[spots[1]].set(high)


def block_scale(stream_key, extent, shards, least, largest):
    factor_of, own = 1.0, jax.random.fold_in(stream_key, 6)
    for position, blocks in shards:
        heights = jnp.exp(jax.random.uniform(jax.random.fold_in(own, position), (blocks,), jnp.float32, least / len(shards), largest / len(shards)))
        factor_of = factor_of * jnp.repeat(heights, extent[position] // blocks).reshape([-1 if axis == position else 1 for axis in range(len(extent))])
    return factor_of


def scatter_about(rng, shape, spread, bound, cuts=(), kind=jnp.bfloat16):
    level = block_scale(rng, shape, cuts, -0.22, 0.18) if cuts else 1.0
    values = jax.random.normal(rng, shape, jnp.float32) * spread * level
    return jnp.minimum(jnp.maximum(values, -bound), bound).astype(kind)


def setup_inputs(seed: int = 0, part: int = 0) -> dict:
    key_of = jax.random.split(jax.random.key(seed), 10)
    part_keys = jax.random.split(jax.random.fold_in(key_of[9], part), 10)
    return {
        "aligned_chain_embedding": scatter_about(part_keys[0], (ALIGNED_CHAINS, WINDOW_AMINOS, ROW_FEATURES), 1.0, 6.0, ((0, 2), (1, 8))),
        "alignment_mask": draw_alignment_mask(jax.random.fold_in(jax.random.fold_in(key_of[9], part), 71), part),
        "resolved_residue_mask": set_ends((jax.random.randint(part_keys[2], (WINDOW_AMINOS,), 0, 5) < 4).astype(jnp.int32), jax.random.fold_in(part_keys[2], 1), 0, 1),
        "pairwise_state": draw_pairwise_state(jax.random.fold_in(jax.random.fold_in(key_of[9], part), 71), part),
        "combined_projection_matrix": scatter_about(key_of[4], (ROW_FEATURES, 4 * ROW_FEATURES), ROW_FEATURES ** -0.5, 0.375),
        "pair_bias_weight": draw_pair_bias_weight(jax.random.fold_in(key_of[9], 71), part),
        "final_projection_matrix": scatter_about(key_of[6], (ROW_FEATURES, ROW_FEATURES), ROW_FEATURES ** -0.5, 0.375),
        "left_right_projection_matrix": scatter_about(key_of[7], (ROW_FEATURES, 2 * PROJ_FEATURES), (ROW_FEATURES // 16) ** -0.5, 1.5),
        "outer_mean_weight": scatter_about(key_of[8], (PROJ_FEATURES * PROJ_FEATURES, CZ), (PROJ_FEATURES * PROJ_FEATURES) ** -0.5, 0.1875),
    }


epsilon = 1e-05

def layer_normalize(values):
    values = values.astype(jnp.float32)
    average = lax.optimization_barrier(jnp.mean(values, axis=-1, keepdims=True))
    centered = values - average
    variance = lax.optimization_barrier(jnp.mean(centered * centered, axis=-1, keepdims=True))
    return centered * lax.rsqrt(variance + epsilon)

def reference(aligned_chain_embedding, alignment_mask, resolved_residue_mask, pairwise_state, combined_projection_matrix, pair_bias_weight, final_projection_matrix, left_right_projection_matrix, outer_mean_weight):
    standardized_rows = layer_normalize(aligned_chain_embedding).astype(jnp.bfloat16)
    linear_mapped = jnp.dot(standardized_rows.reshape(ALIGNED_CHAINS * WINDOW_AMINOS, ROW_FEATURES), combined_projection_matrix, preferred_element_type=jnp.float32)
    linear_mapped = linear_mapped.reshape(ALIGNED_CHAINS, WINDOW_AMINOS, 4, HEAD_NUMBER, PER_HEAD_DIM)
    queries = (linear_mapped[:, :, 0] * PER_HEAD_DIM ** (-0.5)).astype(jnp.bfloat16)
    key_rows = linear_mapped[:, :, 1].astype(jnp.bfloat16)
    value_rows = linear_mapped[:, :, 2].astype(jnp.bfloat16)
    sigmoid_factor = jax.nn.sigmoid(linear_mapped[:, :, 3])
    pair_normed = layer_normalize(pairwise_state).astype(jnp.bfloat16)
    head_bias = jnp.dot(pair_normed.reshape(WINDOW_AMINOS * WINDOW_AMINOS, CZ), pair_bias_weight, preferred_element_type=jnp.float32)
    head_bias = jnp.transpose(head_bias.astype(jnp.bfloat16).reshape(WINDOW_AMINOS, WINDOW_AMINOS, HEAD_NUMBER), (2, 0, 1)).astype(jnp.float32)
    key_validity_mask = (alignment_mask.astype(jnp.float32) - 1.0) * 1000000000.0

    def attend(inputs):
        query_one, key_one, value_one, mask_one = inputs
        scores = jnp.einsum('ihd,jhd->hij', query_one.astype(jnp.float32), key_one.astype(jnp.float32), precision=lax.Precision.HIGHEST)
        scores = scores + head_bias + mask_one[None, None, :]
        row_max = lax.optimization_barrier(jnp.max(scores, axis=-1, keepdims=True))
        exponent = jnp.exp(scores - row_max)
        weights = (exponent / lax.optimization_barrier(jnp.sum(exponent, axis=-1, keepdims=True))).astype(jnp.bfloat16)
        result = jnp.einsum('hij,jhd->ihd', weights.astype(jnp.float32), value_one.astype(jnp.float32), precision=lax.Precision.HIGHEST)
        return result.astype(jnp.bfloat16)
    softmax_mixed = lax.map(attend, (queries, key_rows, value_rows, key_validity_mask))
    sigmoid_scaled = (sigmoid_factor * softmax_mixed.astype(jnp.float32)).astype(jnp.bfloat16).reshape(ALIGNED_CHAINS * WINDOW_AMINOS, ROW_FEATURES)
    embedding_increment = jnp.dot(sigmoid_scaled, final_projection_matrix, preferred_element_type=jnp.float32).reshape(ALIGNED_CHAINS, WINDOW_AMINOS, ROW_FEATURES)
    alignment_output = (aligned_chain_embedding.astype(jnp.float32) + embedding_increment).astype(jnp.bfloat16)
    standardized_product = layer_normalize(alignment_output).astype(jnp.bfloat16)
    left_right_vectors = jnp.dot(standardized_product.reshape(ALIGNED_CHAINS * WINDOW_AMINOS, ROW_FEATURES), left_right_projection_matrix, preferred_element_type=jnp.float32).reshape(ALIGNED_CHAINS, WINDOW_AMINOS, 2, PROJ_FEATURES)
    entry_present = alignment_mask.astype(jnp.float32)[:, :, None]
    left_side = (left_right_vectors[:, :, 0] * entry_present).astype(jnp.bfloat16)
    right_side = (left_right_vectors[:, :, 1] * entry_present).astype(jnp.bfloat16)
    presence_mask_flags = alignment_mask.astype(jnp.bfloat16)
    counts = jnp.dot(presence_mask_flags.T, presence_mask_flags, preferred_element_type=jnp.float32)
    project = outer_mean_weight.astype(jnp.float32)
    block_rows = math.gcd(32, WINDOW_AMINOS)

    def outer_block(start):
        left_piece = lax.dynamic_slice_in_dim(left_side, start, block_rows, 1)
        product = jnp.einsum('sic,sje->ijce', left_piece.astype(jnp.float32), right_side.astype(jnp.float32), precision=lax.Precision.HIGHEST)
        flattened = product.reshape(block_rows * WINDOW_AMINOS, PROJ_FEATURES * PROJ_FEATURES)
        return jnp.dot(flattened, project, precision=lax.Precision.HIGHEST).reshape(block_rows, WINDOW_AMINOS, CZ)
    starts = jnp.arange(WINDOW_AMINOS // block_rows, dtype=jnp.int32) * block_rows
    outer = lax.map(outer_block, starts).reshape(WINDOW_AMINOS, WINDOW_AMINOS, CZ)
    pair_mask = (resolved_residue_mask[:, None] * resolved_residue_mask[None, :]).astype(jnp.float32)
    pairwise_output = (pairwise_state.astype(jnp.float32) + pair_mask[:, :, None] * (outer / counts[:, :, None])).astype(jnp.bfloat16)
    return (alignment_output, pairwise_output)
```

```python
import functools
import math

import jax
import jax.numpy as jnp
from jax import lax
from jax.experimental import pallas as pl
from jax.experimental.pallas import tpu as pltpu
from jax.sharding import PartitionSpec as P

ROW_FEATURES = 256
CZ = 128
HEAD_NUMBER = 8
PER_HEAD_DIM = 32
PROJ_FEATURES = 32


epsilon = 1e-05


def layer_normalize(values):
    values = values.astype(jnp.float32)
    average = jnp.mean(values, axis=-1, keepdims=True)
    centered = values - average
    variance = jnp.mean(centered * centered, axis=-1, keepdims=True)
    return centered * lax.rsqrt(variance + epsilon)


def outer_rows(left_side, right_side, project):
    row_total = left_side.shape[1]
    col_total = right_side.shape[1]
    block_rows = math.gcd(row_total, max(1, 2048 // col_total))

    def outer_block(start):
        product = jnp.einsum(
            "sic,sje->ijce", left_side, right_side, preferred_element_type=jnp.float32
        )
        flattened = product.reshape(block_rows * col_total, PROJ_FEATURES * PROJ_FEATURES)
        return jnp.dot(flattened, project, precision=lax.Precision.HIGHEST).reshape(
            block_rows, col_total, CZ
        )

    starts = jnp.arange(row_total // block_rows, dtype=jnp.int32) * block_rows
    return lax.map(outer_block, starts).reshape(row_total, col_total, CZ)


def per_device(
    aligned_chain_embedding,
    alignment_mask,
    resolved_residue_mask,
    pairwise_state,
    combined_projection_matrix,
    pair_bias_weight,
    final_projection_matrix,
    left_right_projection_matrix,
    outer_mean_weight,
):
    chain_count = aligned_chain_embedding.shape[0]
    amino_count = aligned_chain_embedding.shape[1]
    res_ranks = lax.axis_size("res")
    seq_groups = lax.axis_size("seq")
    full_length = amino_count * res_ranks
    row_count = full_length // seq_groups
    item_count = HEAD_NUMBER * chain_count // res_ranks
    per_head = min(item_count, chain_count)
    head_count = item_count // per_head
    my_rank = lax.axis_index("res")
    my_group = lax.axis_index("seq")
    standardized_rows = layer_normalize(aligned_chain_embedding).astype(jnp.bfloat16)
    linear_mapped = jnp.dot(
        standardized_rows.reshape(chain_count * amino_count, ROW_FEATURES),
        combined_projection_matrix,
        preferred_element_type=jnp.float32,
    )
    linear_mapped = linear_mapped.reshape(chain_count, amino_count, 4, HEAD_NUMBER, PER_HEAD_DIM)
    queries = (linear_mapped[:, :, 0] * PER_HEAD_DIM ** (-0.5)).astype(jnp.bfloat16)
    key_rows = linear_mapped[:, :, 1].astype(jnp.bfloat16)
    value_rows = linear_mapped[:, :, 2].astype(jnp.bfloat16)
    sigmoid_factor = jax.nn.sigmoid(linear_mapped[:, :, 3])
    stacked = jnp.stack([queries, key_rows, value_rows], axis=2)
    stacked = jnp.transpose(stacked, (3, 0, 1, 2, 4)).reshape(
        HEAD_NUMBER * chain_count, amino_count, 3 * PER_HEAD_DIM
    )
    presence_mask_flags = alignment_mask.astype(jnp.bfloat16)
    key_flags = jnp.broadcast_to(
        presence_mask_flags[None], (HEAD_NUMBER, chain_count, amino_count)
    ).reshape(HEAD_NUMBER * chain_count, amino_count)
    arrived, arrived_flags = (
        lax.all_to_all(stacked, "res", split_axis=0, concat_axis=1, tiled=True),
        lax.all_to_all(key_flags, "res", split_axis=0, concat_axis=1, tiled=True),
    )
    pair_normed = layer_normalize(pairwise_state).astype(jnp.bfloat16)
    local_bias = jnp.dot(
        pair_normed.reshape(row_count * amino_count, CZ),
        pair_bias_weight,
        preferred_element_type=jnp.float32,
    )
    local_bias = jnp.transpose(
        local_bias.astype(jnp.bfloat16).reshape(row_count, amino_count, HEAD_NUMBER), (2, 0, 1)
    )
    bias_cols = lax.all_gather(local_bias, "res", axis=2, tiled=True)
    whole_bias = lax.all_gather(bias_cols, "seq", axis=1, tiled=True)
    first_head = my_rank * item_count // chain_count
    head_bias = lax.dynamic_slice_in_dim(whole_bias, first_head, head_count, 0)
    grouped = arrived.reshape(head_count, per_head, full_length, 3, PER_HEAD_DIM)
    key_validity_mask = (
        arrived_flags.reshape(head_count, per_head, full_length).astype(jnp.float32) - 1.0
    ) * 1000000000.0
    scores = jnp.einsum(
        "gpid,gpjd->gpij",
        grouped[:, :, :, 0],
        grouped[:, :, :, 1],
        preferred_element_type=jnp.float32,
    )
    scores = scores + head_bias.astype(jnp.float32)[:, None] + key_validity_mask[:, :, None, :]
    row_max = jnp.max(scores, axis=-1, keepdims=True)
    exponent = jnp.exp(scores - row_max)
    weights = (exponent / jnp.sum(exponent, axis=-1, keepdims=True)).astype(jnp.bfloat16)
    softmax_mixed = jnp.einsum(
        "gpij,gpjd->gpid", weights, grouped[:, :, :, 2], preferred_element_type=jnp.float32
    )
    softmax_mixed = softmax_mixed.astype(jnp.bfloat16).reshape(
        item_count, full_length, PER_HEAD_DIM
    )
    returned = lax.all_to_all(softmax_mixed, "res", split_axis=1, concat_axis=0, tiled=True)
    returned = jnp.transpose(
        returned.reshape(HEAD_NUMBER, chain_count, amino_count, PER_HEAD_DIM), (1, 2, 0, 3)
    )
    sigmoid_scaled = (
        (sigmoid_factor * returned.astype(jnp.float32))
        .astype(jnp.bfloat16)
        .reshape(chain_count * amino_count, ROW_FEATURES)
    )
    embedding_increment = jnp.dot(
        sigmoid_scaled, final_projection_matrix, preferred_element_type=jnp.float32
    ).reshape(chain_count, amino_count, ROW_FEATURES)
    alignment_output = (aligned_chain_embedding.astype(jnp.float32) + embedding_increment).astype(
        jnp.bfloat16
    )
    standardized_product = layer_normalize(alignment_output).astype(jnp.bfloat16)
    left_right_vectors = jnp.dot(
        standardized_product.reshape(chain_count * amino_count, ROW_FEATURES),
        left_right_projection_matrix,
        preferred_element_type=jnp.float32,
    )
    left_right_vectors = left_right_vectors.reshape(chain_count, amino_count, 2, PROJ_FEATURES)
    entry_present = alignment_mask.astype(jnp.float32)[:, :, None]
    left_side = (left_right_vectors[:, :, 0] * entry_present).astype(jnp.bfloat16)
    right_side = (left_right_vectors[:, :, 1] * entry_present).astype(jnp.bfloat16)
    left_all, left_flags = (
        lax.all_gather(left_side, "res", axis=1, tiled=True),
        lax.all_gather(presence_mask_flags, "res", axis=1, tiled=True),
    )
    project = outer_mean_weight.astype(jnp.float32)
    row_start = my_group * row_count
    left_full, flag_full = (
        lax.all_to_all(left_all, "seq", split_axis=1, concat_axis=0, tiled=True),
        lax.all_to_all(left_flags, "seq", split_axis=1, concat_axis=0, tiled=True),
    )
    right_full, right_flags = (
        lax.all_gather(right_side, "seq", axis=0, tiled=True),
        lax.all_gather(presence_mask_flags, "seq", axis=0, tiled=True),
    )
    counts = jnp.dot(flag_full.T, right_flags, preferred_element_type=jnp.float32)
    outer = outer_rows(left_full, right_full, project)
    col_start = my_rank * amino_count
    row_mask = lax.dynamic_slice_in_dim(resolved_residue_mask, row_start, row_count).astype(
        jnp.float32
    )
    col_mask = lax.dynamic_slice_in_dim(resolved_residue_mask, col_start, amino_count).astype(
        jnp.float32
    )
    pair_mask = row_mask[:, None] * col_mask[None, :]
    pairwise_output = (
        pairwise_state.astype(jnp.float32) + pair_mask[:, :, None] * (outer / counts[:, :, None])
    ).astype(jnp.bfloat16)
    return (alignment_output, pairwise_output)


LANES = 128
F32 = jnp.float32
BF16 = jnp.bfloat16


def iota(shape, axis):
    return lax.broadcasted_iota(jnp.int32, shape, axis)


def dot(a, b, ca=1, cb=0):
    return lax.dot_general(a, b, (((ca,), (cb,)), ((), ())), preferred_element_type=F32)


def one_hot(cond):
    return jnp.where(cond, 1.0, 0.0).astype(BF16)


def flat(block):
    return block.reshape(-1, block.shape[-1])


def fused_kernel(
    groups, ranks, per, aminos,
    emb_hbm, mask_hbm, resolved_hbm, pair_hbm, proj_hbm, bias_hbm, final_hbm, lr_hbm, outer_hbm,
    out_ref, pair_out_ref,
    emb_in, mask_ref, resolved_ref, pair_ref, proj_ref, bias_w_ref, final_ref, lr_ref, outer_ref,
    emb_buf, flag_buf, bias_buf, left_send, right_send, left_buf, right_buf, out_send,
    product_buf, lhs_buf, turn_buf,
    load_s, emb_s, emb_r, out_s, out_r,
    flag_s, flag_r, bias_s, bias_r, left_s, left_r, right_s, right_r,
):
    devices = groups * ranks
    chains = per * ranks
    full = ranks * aminos
    rows = per * full
    pair_rows = full // groups
    pairs = pair_rows * aminos
    quads = pair_rows // aminos
    width = HEAD_NUMBER * PER_HEAD_DIM
    halves = width // LANES
    heads_per = LANES // PER_HEAD_DIM
    slot = LANES // groups
    group = lax.axis_index("seq")
    rank = lax.axis_index("res")
    me = group * ranks + rank

    def flip(k):
        peer = 0
        for bit in range(ranks.bit_length() - 1):
            digit = rank // (1 << bit) % 2
            peer = peer + (1 << bit) * (1 - digit if k >> bit & 1 else digit)
        return peer

    others = []
    for shift in range(groups - 1, -1, -1):
        for k in range(ranks - 1, -1, -1):
            if shift or k:
                others.append((shift * ranks + k, lax.rem(group + shift, groups), flip(k)))

    def where_is(g, r):
        return {"seq": g, "res": r}

    barrier = pltpu.get_barrier_semaphore()
    for _, g, r in others:
        pl.semaphore_signal(
            barrier, inc=1, device_id=where_is(g, r), device_id_type=pl.DeviceIdType.MESH
        )

    def load(k, src, dst):
        copy = pltpu.make_async_copy(src, dst, load_s.at[k])
        copy.start()
        return copy

    pair_load = load(0, pair_hbm, pair_ref)
    bias_load = load(1, bias_hbm, bias_w_ref)
    mask_load = load(2, mask_hbm, mask_ref)
    emb_load = load(3, emb_hbm, emb_in)
    proj_load = load(4, proj_hbm, proj_ref)
    final_load = load(5, final_hbm, final_ref)
    lr_load = load(6, lr_hbm, lr_ref)
    outer_load = load(7, outer_hbm, outer_ref)
    resolved_load = load(8, resolved_hbm, resolved_ref)

    def send(src, dst, ssem, rsem, device):
        copy = pltpu.make_async_remote_copy(
            src_ref=src, dst_ref=dst, send_sem=ssem, recv_sem=rsem,
            device_id=device, device_id_type=pl.DeviceIdType.MESH,
        )
        copy.start()
        return copy

    def take(view, sem):
        pltpu.make_async_copy(view, view, sem).wait()

    rest, near_rest = pl.ds(0, devices - 1), pl.ds(0, per * (ranks - 1))
    bias_all, flag_all, right_all = bias_buf.at[rest], flag_buf.at[rest], right_buf.at[rest]
    left_all = left_buf.at[:, rest]
    emb_all, out_all = emb_in.at[near_rest], out_ref.at[near_rest]

    bias_load.wait()
    lane_head = iota((LANES, HEAD_NUMBER), 0)
    lane_head = (lane_head // slot + group) % groups * heads_per + lane_head % slot // pair_rows
    wide_w = dot(one_hot(lane_head == iota((LANES, HEAD_NUMBER), 1)), bias_w_ref[...]).astype(BF16)
    mask_load.wait()
    flags = dot(mask_ref[...].astype(F32).astype(BF16), one_hot(
        iota((chains, LANES), 0) == iota((chains, LANES), 1)))
    flag_buf[me] = flags.astype(BF16)
    pair_load.wait()
    pair_value = flat(pair_ref[...].astype(F32))
    own_bias = dot(layer_normalize(pair_value).astype(BF16), wide_w, 1, 1)
    own_bias = jnp.where(
        iota((pairs, LANES), 0) // aminos == iota((pairs, LANES), 1) % pair_rows, own_bias, 0.0)
    own_bias = jnp.sum(own_bias.reshape(pair_rows, aminos, LANES), axis=0)
    bias_buf[me] = own_bias.astype(BF16)
    own = pl.ds(rank * per, per)
    emb_load.wait()
    emb_buf[:, pl.ds(rank, 1)] = emb_in[own][:, None]

    pl.semaphore_wait(barrier, devices - 1)
    for k, g, r in others:
        send(bias_buf.at[me], bias_buf.at[me], bias_s, bias_r,
                                where_is(g, r))
    for k, g, r in others:
        if k < ranks:
            send(emb_in.at[pl.ds(r * per, per)], emb_buf.at[:, rank],
                                   emb_s, emb_r, where_is(g, r))
    for k, g, r in others[::-1]:
        send(flag_buf.at[me], flag_buf.at[me], flag_s, flag_r,
                                where_is(g, r))

    heads_q = heads_per * pair_rows
    block_mask = (iota((LANES, LANES), 0) % slot // pair_rows
                  == iota((LANES, LANES), 1) // PER_HEAD_DIM)
    take(emb_all, emb_r)
    embedding = emb_buf[...].astype(F32).reshape(rows, ROW_FEATURES)
    normed = layer_normalize(embedding).astype(BF16)
    proj_load.wait()
    projected = dot(normed, proj_ref[...])
    queries = (projected[:, :width] * PER_HEAD_DIM ** (-0.5)).astype(BF16)
    keys = projected[:, width:2 * width].astype(BF16)
    values = projected[:, 2 * width:3 * width].astype(BF16)
    gating = jax.nn.sigmoid(projected[:, 3 * width:])

    raw = {}
    for b in range(halves):
        cols = slice(b * LANES, (b + 1) * LANES)
        for c in range(per):
            spread = []
            for s in range(groups):
                at = c * full + (b - s) % groups * pair_rows
                spread += [queries[at:at + pair_rows, cols]] * heads_per
            spread = jnp.concatenate(spread, axis=0)
            spread = jnp.where(block_mask, spread, jnp.zeros_like(spread))
            raw[b, c] = dot(keys[c * full:(c + 1) * full, cols], spread, 1, 1)

    take(flag_all, flag_r)
    near = flat(flag_buf[pl.ds(group * ranks, ranks)])
    pick = one_hot(iota((LANES, per * LANES), 0)
                   == rank * per + iota((LANES, per * LANES), 1) // LANES)
    key_flags = dot(near, pick)
    key_mask = (key_flags - 1.0) * 1000000000.0
    present = jnp.concatenate(
        [key_flags[:, c * LANES:(c + 1) * LANES] for c in range(per)], axis=0)

    take(bias_all, bias_r)
    bias = [flat(bias_buf[pl.ds(g * ranks, ranks)]).astype(F32) for g in range(groups)]
    which = iota((full, LANES), 1) // slot
    mixed = []
    for b in range(halves):
        cols = slice(b * LANES, (b + 1) * LANES)
        tile_bias = bias[b % groups]
        for s in range(1, groups):
            tile_bias = jnp.where(which == s, bias[(b - s) % groups], tile_bias)
        weights, blocks = [], []
        for c in range(per):
            scores = raw[b, c] + tile_bias + key_mask[:, c * LANES:(c + 1) * LANES]
            exponent = jnp.exp(scores - jnp.max(scores, axis=0, keepdims=True))
            total = 1.0 / jnp.sum(exponent, axis=0, keepdims=True)
            weights.append((exponent * total).astype(BF16))
            own_values = values[c * full:(c + 1) * full, cols]
            blocks.append(jnp.concatenate(
                [own_values if d == c else jnp.zeros_like(own_values) for d in range(per)], axis=1))
        weights = jnp.concatenate(weights, axis=0)
        blocks = jnp.concatenate(blocks, axis=0)
        summed = dot(weights, blocks, 0, 0)
        lane_h = iota((pair_rows, LANES), 1) // PER_HEAD_DIM
        parts = []
        for c in range(per):
            for g in range(groups):
                at = (b - g) % groups * slot
                part = summed[at:at + pair_rows, c * LANES:(c + 1) * LANES]
                for h in range(1, heads_per):
                    row = at + h * pair_rows
                    part = jnp.where(
                        lane_h == h,
                        summed[row:row + pair_rows, c * LANES:(c + 1) * LANES], part)
                parts.append(part)
        mixed.append(jnp.concatenate(parts, axis=0))
    attended = jnp.concatenate(mixed, axis=1).astype(BF16)
    gated = (gating * attended.astype(F32)).astype(BF16)
    final_load.wait()
    lr_load.wait()
    updated = (embedding + dot(gated, final_ref[...])).astype(BF16)
    normed_out = layer_normalize(updated).astype(BF16)
    sides_w = jnp.concatenate(
        [lr_ref[:PROJ_FEATURES, :]] * aminos + [lr_ref[PROJ_FEATURES:, :]] * aminos, axis=0)
    sides = dot(normed_out, sides_w, 1, 1)
    two = (rows, 2 * LANES)
    sides = (sides * jnp.concatenate([present] * 2, axis=1)).astype(BF16)
    sides = jnp.where(iota(two, 1) // PROJ_FEATURES % aminos == iota(two, 0) % aminos,
                      sides, jnp.zeros_like(sides))
    sq = (chains, rows)
    gather = one_hot((iota(sq, 0) // per == iota(sq, 1) % full // aminos)
                     & (iota(sq, 0) % per == iota(sq, 1) // full))
    sides = dot(gather, sides).reshape(ranks, per, 2 * LANES).astype(BF16)
    left_send[...] = sides[:, :, :LANES]
    right_send[...] = sides[:, :, LANES:]
    for k, g, r in others:
        send(left_send.at[pl.ds(g * quads, quads)], left_buf.at[:, me],
                                left_s, left_r, where_is(g, r))
        send(right_send.at[r], right_buf.at[me],
                                 right_s, right_r, where_is(g, r))
    out_send[...] = updated.astype(F32).reshape(per, ranks, aminos, ROW_FEATURES).astype(BF16)
    for k, g, r in others:
        if k < ranks:
            send(out_send.at[:, r], out_ref.at[own],
                                   out_s, out_r, where_is(g, r))
    left_buf[:, pl.ds(me, 1)] = left_send[pl.ds(group * quads, quads)][:, None]
    right_buf[me] = right_send[rank]
    out_ref[own] = out_send[:, pl.ds(rank, 1)].reshape(per, aminos, ROW_FEATURES)

    at = (pairs, full)
    row_pick = iota(at, 1) == group * pair_rows + iota(at, 0) // aminos
    col_pick = iota(at, 1) == rank * aminos + iota(at, 0) % aminos
    both = jnp.zeros((pairs, LANES), F32)
    for g in range(groups):
        seen = flat(flag_buf[pl.ds(g * ranks, ranks)])
        both = both + dot(one_hot(row_pick), seen) * dot(one_hot(col_pick), seen)
    counts = jnp.sum(both, axis=1, keepdims=True)
    resolved_load.wait()
    resolved = jnp.broadcast_to(resolved_ref[...].astype(F32), at)
    scale = jnp.sum(jnp.where(row_pick, resolved, 0.0), axis=1, keepdims=True) * jnp.sum(
        jnp.where(col_pick, resolved, 0.0), axis=1, keepdims=True) / counts
    scale = jnp.broadcast_to(scale, (pairs, LANES))
    outer_load.wait()
    block = iota((pair_rows, LANES), 1) // PROJ_FEATURES
    take(right_all, right_r)
    take(left_all, left_r)
    right_rows = flat(right_buf[...])
    for q in range(quads):
        product_buf[q * LANES:(q + 1) * LANES, :] = dot(flat(left_buf[q]), right_rows, 0, 0)
    for c in range(0, PROJ_FEATURES, aminos):
        slabs = [product_buf[pl.ds(c + x, pair_rows, stride=PROJ_FEATURES), :]
                 for x in range(aminos)]
        for j in range(aminos):
            turned = jnp.zeros((pair_rows, LANES), F32)
            for x in range(aminos):
                shift = (x - j) % aminos * PROJ_FEATURES
                moved = pltpu.roll(slabs[x], shift, 1) if shift else slabs[x]
                turned = jnp.where(block == x, moved, turned)
            lhs_buf[j * pair_rows:(j + 1) * pair_rows,
                    c * PROJ_FEATURES:c * PROJ_FEATURES + LANES] = turned.astype(BF16)
    outer = dot(lhs_buf[...], outer_ref[...])
    for j in range(aminos):
        turn_buf[pl.ds(j, pair_rows, stride=aminos), :] = outer[j * pair_rows:(j + 1) * pair_rows]
    result = pair_value + scale * turn_buf[...]
    pair_out_ref[...] = result.reshape(pair_rows, aminos, CZ).astype(BF16)
    take(out_all, out_r)
    for view, sem in ((bias_all, bias_s), (emb_all, emb_s), (flag_all, flag_s),
                      (left_all, left_s), (right_all, right_s), (out_all, out_s)):
        take(view, sem)


def write_kernel(out_ref, pair_ref, out_hbm, pair_hbm, sem):
    copies = [pltpu.make_async_copy(out_ref, out_hbm, sem.at[0]),
              pltpu.make_async_copy(pair_ref, pair_hbm, sem.at[1])]
    for copy in copies:
        copy.start()
    for copy in copies:
        copy.wait()


def fused(*args):
    emb, mask, resolved, pair = args[:4]
    groups, ranks = lax.axis_size("seq"), lax.axis_size("res")
    chains, aminos = emb.shape[:2]
    per = chains // ranks
    pair_rows = pair.shape[0]
    quads = pair_rows // aminos
    devices = groups * ranks
    operands = (emb, mask.T, resolved.reshape(1, -1), pair, args[4], args[5].T, args[6],
                args[7].T, args[8])
    vmem = pl.BlockSpec(memory_space=pltpu.VMEM)
    whole = pl.BlockSpec(memory_space=pl.ANY)
    dma = pltpu.SemaphoreType.DMA
    results = pl.pallas_call(
        functools.partial(fused_kernel, groups, ranks, per, aminos),
        out_shape=(pltpu.VMEM(emb.shape, BF16), pltpu.VMEM(pair.shape, BF16)),
        in_specs=[whole] * len(operands),
        out_specs=(vmem, vmem),
        scratch_shapes=[pltpu.VMEM(x.shape, x.dtype) for x in operands] + [
            pltpu.VMEM((per, ranks, aminos, ROW_FEATURES), BF16),
            pltpu.VMEM((devices, aminos, LANES), BF16),
            pltpu.VMEM((devices, aminos, LANES), BF16),
            pltpu.VMEM((ranks, per, LANES), BF16),
            pltpu.VMEM((ranks, per, LANES), BF16),
            pltpu.VMEM((quads, devices, per, LANES), BF16),
            pltpu.VMEM((devices, per, LANES), BF16),
            pltpu.VMEM((per, ranks, aminos, ROW_FEATURES), BF16),
            pltpu.VMEM((pair_rows * PROJ_FEATURES, LANES), F32),
            pltpu.VMEM((pair_rows * aminos, PROJ_FEATURES * PROJ_FEATURES), BF16),
            pltpu.VMEM((pair_rows * aminos, CZ), F32),
            dma((len(operands),)),
        ] + [dma] * 12,
        compiler_params=pltpu.CompilerParams(collective_id=0, has_side_effects=True),
    )(*operands)
    return pl.pallas_call(
        write_kernel,
        out_shape=(jax.ShapeDtypeStruct(emb.shape, BF16), jax.ShapeDtypeStruct(pair.shape, BF16)),
        in_specs=[whole, whole],
        out_specs=(whole, whole),
        scratch_shapes=[dma((2,))],
    )(*[pltpu.with_memory_space_constraint(x, pltpu.VMEM) for x in results])


def fits(mesh, emb, pair):
    groups, ranks = mesh.shape["seq"], mesh.shape["res"]
    chains, aminos = emb.shape[:2]
    if chains % ranks or aminos * PROJ_FEATURES != LANES or chains * aminos != LANES:
        return False
    if ranks & (ranks - 1) or HEAD_NUMBER * PER_HEAD_DIM != groups * LANES:
        return False
    pairs = pair.shape[0] * aminos
    return pairs * groups == LANES and chains // ranks * aminos * groups == PROJ_FEATURES


def solution(mesh):
    placed = (
        P(("crop", "seq"), "res", None),
        P(("crop", "seq"), "res"),
        P("crop"),
        P(("crop", "seq"), "res", None),
        P(),
        P(),
        P(),
        P(),
        P(),
    )
    def either(*args):
        return (fused if fits(mesh, args[0], args[3]) else per_device)(*args)

    return jax.shard_map(
        either,
        mesh=mesh,
        in_specs=placed,
        out_specs=(P(("crop", "seq"), "res", None), P(("crop", "seq"), "res", None)),
        check_vma=False,
    )
```

```python
import functools
import math

import jax
import jax.numpy as jnp
from jax import lax
from jax.experimental import pallas as pl
from jax.experimental.pallas import tpu as pltpu
from jax.sharding import PartitionSpec as P

ROW_FEATURES = 256
CZ = 128
HEAD_NUMBER = 8
PER_HEAD_DIM = 32
PROJ_FEATURES = 32


epsilon = 1e-05


def layer_normalize(values):
    values = values.astype(jnp.float32)
    average = jnp.mean(values, axis=-1, keepdims=True)
    centered = values - average
    variance = jnp.mean(centered * centered, axis=-1, keepdims=True)
    return centered * lax.rsqrt(variance + epsilon)


def outer_rows(left_side, right_side, project):
    row_total = left_side.shape[1]
    col_total = right_side.shape[1]
    block_rows = math.gcd(row_total, max(1, 2048 // col_total))

    def outer_block(start):
        product = jnp.einsum(
            "sic,sje->ijce", left_side, right_side, preferred_element_type=jnp.float32
        )
        flattened = product.reshape(block_rows * col_total, PROJ_FEATURES * PROJ_FEATURES)
        return jnp.dot(flattened, project, precision=lax.Precision.HIGHEST).reshape(
            block_rows, col_total, CZ
        )

    starts = jnp.arange(row_total // block_rows, dtype=jnp.int32) * block_rows
    return lax.map(outer_block, starts).reshape(row_total, col_total, CZ)


def per_device(
    aligned_chain_embedding,
    alignment_mask,
    resolved_residue_mask,
    pairwise_state,
    combined_projection_matrix,
    pair_bias_weight,
    final_projection_matrix,
    left_right_projection_matrix,
    outer_mean_weight,
):
    chain_count = aligned_chain_embedding.shape[0]
    amino_count = aligned_chain_embedding.shape[1]
    res_ranks = lax.axis_size("res")
    seq_groups = lax.axis_size("seq")
    full_length = amino_count * res_ranks
    row_count = full_length // seq_groups
    item_count = HEAD_NUMBER * chain_count // res_ranks
    per_head = min(item_count, chain_count)
    head_count = item_count // per_head
    my_rank = lax.axis_index("res")
    my_group = lax.axis_index("seq")
    standardized_rows = layer_normalize(aligned_chain_embedding).astype(jnp.bfloat16)
    linear_mapped = jnp.dot(
        standardized_rows.reshape(chain_count * amino_count, ROW_FEATURES),
        combined_projection_matrix,
        preferred_element_type=jnp.float32,
    )
    linear_mapped = linear_mapped.reshape(chain_count, amino_count, 4, HEAD_NUMBER, PER_HEAD_DIM)
    queries = (linear_mapped[:, :, 0] * PER_HEAD_DIM ** (-0.5)).astype(jnp.bfloat16)
    key_rows = linear_mapped[:, :, 1].astype(jnp.bfloat16)
    value_rows = linear_mapped[:, :, 2].astype(jnp.bfloat16)
    sigmoid_factor = jax.nn.sigmoid(linear_mapped[:, :, 3])
    stacked = jnp.stack([queries, key_rows, value_rows], axis=2)
    stacked = jnp.transpose(stacked, (3, 0, 1, 2, 4)).reshape(
        HEAD_NUMBER * chain_count, amino_count, 3 * PER_HEAD_DIM
    )
    presence_mask_flags = alignment_mask.astype(jnp.bfloat16)
    key_flags = jnp.broadcast_to(
        presence_mask_flags[None], (HEAD_NUMBER, chain_count, amino_count)
    ).reshape(HEAD_NUMBER * chain_count, amino_count)
    arrived, arrived_flags = (
        lax.all_to_all(stacked, "res", split_axis=0, concat_axis=1, tiled=True),
        lax.all_to_all(key_flags, "res", split_axis=0, concat_axis=1, tiled=True),
    )
    pair_normed = layer_normalize(pairwise_state).astype(jnp.bfloat16)
    local_bias = jnp.dot(
        pair_normed.reshape(row_count * amino_count, CZ),
        pair_bias_weight,
        preferred_element_type=jnp.float32,
    )
    local_bias = jnp.transpose(
        local_bias.astype(jnp.bfloat16).reshape(row_count, amino_count, HEAD_NUMBER), (2, 0, 1)
    )
    bias_cols = lax.all_gather(local_bias, "res", axis=2, tiled=True)
    whole_bias = lax.all_gather(bias_cols, "seq", axis=1, tiled=True)
    first_head = my_rank * item_count // chain_count
    head_bias = lax.dynamic_slice_in_dim(whole_bias, first_head, head_count, 0)
    grouped = arrived.reshape(head_count, per_head, full_length, 3, PER_HEAD_DIM)
    key_validity_mask = (
        arrived_flags.reshape(head_count, per_head, full_length).astype(jnp.float32) - 1.0
    ) * 1000000000.0
    scores = jnp.einsum(
        "gpid,gpjd->gpij",
        grouped[:, :, :, 0],
        grouped[:, :, :, 1],
        preferred_element_type=jnp.float32,
    )
    scores = scores + head_bias.astype(jnp.float32)[:, None] + key_validity_mask[:, :, None, :]
    row_max = jnp.max(scores, axis=-1, keepdims=True)
    exponent = jnp.exp(scores - row_max)
    weights = (exponent / jnp.sum(exponent, axis=-1, keepdims=True)).astype(jnp.bfloat16)
    softmax_mixed = jnp.einsum(
        "gpij,gpjd->gpid", weights, grouped[:, :, :, 2], preferred_element_type=jnp.float32
    )
    softmax_mixed = softmax_mixed.astype(jnp.bfloat16).reshape(
        item_count, full_length, PER_HEAD_DIM
    )
    returned = lax.all_to_all(softmax_mixed, "res", split_axis=1, concat_axis=0, tiled=True)
    returned = jnp.transpose(
        returned.reshape(HEAD_NUMBER, chain_count, amino_count, PER_HEAD_DIM), (1, 2, 0, 3)
    )
    sigmoid_scaled = (
        (sigmoid_factor * returned.astype(jnp.float32))
        .astype(jnp.bfloat16)
        .reshape(chain_count * amino_count, ROW_FEATURES)
    )
    embedding_increment = jnp.dot(
        sigmoid_scaled, final_projection_matrix, preferred_element_type=jnp.float32
    ).reshape(chain_count, amino_count, ROW_FEATURES)
    alignment_output = (aligned_chain_embedding.astype(jnp.float32) + embedding_increment).astype(
        jnp.bfloat16
    )
    standardized_product = layer_normalize(alignment_output).astype(jnp.bfloat16)
    left_right_vectors = jnp.dot(
        standardized_product.reshape(chain_count * amino_count, ROW_FEATURES),
        left_right_projection_matrix,
        preferred_element_type=jnp.float32,
    )
    left_right_vectors = left_right_vectors.reshape(chain_count, amino_count, 2, PROJ_FEATURES)
    entry_present = alignment_mask.astype(jnp.float32)[:, :, None]
    left_side = (left_right_vectors[:, :, 0] * entry_present).astype(jnp.bfloat16)
    right_side = (left_right_vectors[:, :, 1] * entry_present).astype(jnp.bfloat16)
    left_all, left_flags = (
        lax.all_gather(left_side, "res", axis=1, tiled=True),
        lax.all_gather(presence_mask_flags, "res", axis=1, tiled=True),
    )
    project = outer_mean_weight.astype(jnp.float32)
    row_start = my_group * row_count
    left_full, flag_full = (
        lax.all_to_all(left_all, "seq", split_axis=1, concat_axis=0, tiled=True),
        lax.all_to_all(left_flags, "seq", split_axis=1, concat_axis=0, tiled=True),
    )
    right_full, right_flags = (
        lax.all_gather(right_side, "seq", axis=0, tiled=True),
        lax.all_gather(presence_mask_flags, "seq", axis=0, tiled=True),
    )
    counts = jnp.dot(flag_full.T, right_flags, preferred_element_type=jnp.float32)
    outer = outer_rows(left_full, right_full, project)
    col_start = my_rank * amino_count
    row_mask = lax.dynamic_slice_in_dim(resolved_residue_mask, row_start, row_count).astype(
        jnp.float32
    )
    col_mask = lax.dynamic_slice_in_dim(resolved_residue_mask, col_start, amino_count).astype(
        jnp.float32
    )
    pair_mask = row_mask[:, None] * col_mask[None, :]
    pairwise_output = (
        pairwise_state.astype(jnp.float32) + pair_mask[:, :, None] * (outer / counts[:, :, None])
    ).astype(jnp.bfloat16)
    return (alignment_output, pairwise_output)


LANES = 128
F32 = jnp.float32
BF16 = jnp.bfloat16


def iota(shape, axis):
    return lax.broadcasted_iota(jnp.int32, shape, axis)


def dot(a, b, ca=1, cb=0):
    return lax.dot_general(a, b, (((ca,), (cb,)), ((), ())), preferred_element_type=F32)


def one_hot(cond):
    return jnp.where(cond, 1.0, 0.0).astype(BF16)


def flat(block):
    return block.reshape(-1, block.shape[-1])


def fused_kernel(
    groups, ranks, per, aminos,
    emb_hbm, mask_hbm, resolved_hbm, pair_hbm, proj_hbm, bias_hbm, final_hbm, lr_hbm, outer_hbm,
    out_ref, pair_out_ref,
    pack, near, far, mask_ref, resolved_ref, pair_ref, proj_ref, bias_w_ref, final_ref, lr_ref,
    outer_ref, side_send, side_buf, out_send, raw_buf, mask_buf, gate_buf, value_buf,
    product_buf, turn_buf, load_s, send_s, near_r, far_r, side_r, out_r,
):
    devices = groups * ranks
    chains = per * ranks
    full = ranks * aminos
    rows = per * full
    pair_rows = full // groups
    pairs = pair_rows * aminos
    quads = pair_rows // aminos
    width = HEAD_NUMBER * PER_HEAD_DIM
    halves = width // LANES
    heads_per = LANES // PER_HEAD_DIM
    slot = LANES // groups
    group = lax.axis_index("seq")
    rank = lax.axis_index("res")
    me = group * ranks + rank

    def flip(k):
        peer = 0
        for bit in range(ranks.bit_length() - 1):
            digit = rank // (1 << bit) % 2
            peer = peer + (1 << bit) * (1 - digit if k >> bit & 1 else digit)
        return peer

    others = []
    for shift in range(groups - 1, -1, -1):
        for k in range(ranks - 1, -1, -1):
            if shift or k:
                others.append((shift * ranks + k, lax.rem(group + shift, groups), flip(k)))

    barrier = pltpu.get_barrier_semaphore()
    for _, g, r in others:
        pl.semaphore_signal(
            barrier, inc=1, device_id={"seq": g, "res": r}, device_id_type=pl.DeviceIdType.MESH
        )

    def load(k, src, dst):
        copy = pltpu.make_async_copy(src, dst, load_s.at[k])
        copy.start()
        return copy

    emb_load = load(0, emb_hbm, pack.at[:, pl.ds(0, per)])
    pair_load = load(1, pair_hbm, pair_ref)
    bias_load = load(2, bias_hbm, bias_w_ref)
    mask_load = load(3, mask_hbm, mask_ref)
    proj_load = load(4, proj_hbm, proj_ref)
    final_load = load(5, final_hbm, final_ref)
    lr_load = load(6, lr_hbm, lr_ref)
    resolved_load = load(7, resolved_hbm, resolved_ref)
    for j in range(aminos):
        load(8, outer_hbm, outer_ref.at[:, j])

    def send(src, dst, rsem, g, r):
        pltpu.make_async_remote_copy(
            src_ref=src, dst_ref=dst, send_sem=send_s, recv_sem=rsem,
            device_id={"seq": g, "res": r}, device_id_type=pl.DeviceIdType.MESH,
        ).start()

    def take(view, sem):
        pltpu.make_async_copy(view, view, sem).wait()

    own = pl.ds(rank * per, per)
    near_all = near.at[:, pl.ds(0, ranks - 1)]
    side_all = side_buf.at[:, pl.ds(0, devices - 1)]
    out_all = out_ref.at[pl.ds(0, per * (ranks - 1))]

    bias_load.wait()
    lane_head = iota((LANES, HEAD_NUMBER), 0)
    lane_head = (lane_head // slot + group) % groups * heads_per + lane_head % slot // pair_rows
    wide_w = dot(one_hot(lane_head == iota((LANES, HEAD_NUMBER), 1)), bias_w_ref[...]).astype(BF16)
    mask_load.wait()
    flags = dot(mask_ref[...].astype(F32).astype(BF16), one_hot(
        iota((chains, LANES), 0) == iota((chains, LANES), 1)))
    pair_load.wait()
    pair_value = flat(pair_ref[...].astype(F32))
    own_bias = dot(layer_normalize(pair_value).astype(BF16), wide_w, 1, 1)
    own_bias = jnp.where(
        iota((pairs, LANES), 0) // aminos == iota((pairs, LANES), 1) % pair_rows, own_bias, 0.0)
    own_bias = jnp.sum(own_bias.reshape(pair_rows, aminos, LANES), axis=0)
    aux = jnp.concatenate([own_bias, flags], axis=1).astype(BF16)
    for r in range(ranks):
        pack[r, per] = aux
    emb_load.wait()
    near[:, pl.ds(rank, 1)] = pack[rank][:, None]

    pl.semaphore_wait(barrier, devices - 1)
    for k, g, r in others:
        if k < ranks:
            send(pack.at[r], near.at[:, rank], near_r, g, r)
        else:
            send(pack.at[0, per], far.at[rank], far_r, g, r)

    block_mask = (iota((LANES, LANES), 0) % slot // pair_rows
                  == iota((LANES, LANES), 1) // PER_HEAD_DIM)
    take(near_all, near_r)
    embedding = near[:per].astype(F32).reshape(rows, ROW_FEATURES)
    normed = layer_normalize(embedding).astype(BF16)
    proj_load.wait()
    projected = dot(normed, proj_ref[...])
    queries = (projected[:, :width] * PER_HEAD_DIM ** (-0.5)).astype(BF16)
    keys = projected[:, width:2 * width].astype(BF16)
    value_buf[...] = projected[:, 2 * width:3 * width].astype(BF16)
    gate_buf[...] = jax.nn.sigmoid(projected[:, 3 * width:])

    for b in range(halves):
        cols = slice(b * LANES, (b + 1) * LANES)
        for c in range(per):
            spread = []
            for s in range(groups):
                at = c * full + (b - s) % groups * pair_rows
                spread += [queries[at:at + pair_rows, cols]] * heads_per
            spread = jnp.concatenate(spread, axis=0)
            spread = jnp.where(block_mask, spread, jnp.zeros_like(spread))
            raw_buf[c * full:(c + 1) * full, cols] = dot(
                keys[c * full:(c + 1) * full, cols], spread, 1, 1)

    near_aux = flat(near[per])
    pick = one_hot(iota((LANES, per * LANES), 0)
                   == rank * per + iota((LANES, per * LANES), 1) // LANES)
    key_flags = dot(near_aux[:, LANES:], pick)
    for c in range(per):
        mask_buf[c * full:(c + 1) * full, :] = key_flags[:, c * LANES:(c + 1) * LANES]

    take(far, far_r)
    far_aux = flat(far[...])
    near_bias = near_aux[:, :LANES].astype(F32)
    far_bias = far_aux[:, :LANES].astype(F32)
    which = iota((full, LANES), 1) // slot
    mixed = []
    for b in range(halves):
        cols = slice(b * LANES, (b + 1) * LANES)
        tile_bias = jnp.where((b + which) % groups == group, near_bias, far_bias)
        weights, blocks = [], []
        for c in range(per):
            at = slice(c * full, (c + 1) * full)
            scores = raw_buf[at, cols] + tile_bias + (mask_buf[at, :] - 1.0) * 1000000000.0
            exponent = jnp.exp(scores - jnp.max(scores, axis=0, keepdims=True))
            total = 1.0 / jnp.sum(exponent, axis=0, keepdims=True)
            weights.append((exponent * total).astype(BF16))
            own_values = value_buf[at, cols]
            blocks.append(jnp.concatenate(
                [own_values if d == c else jnp.zeros_like(own_values) for d in range(per)], axis=1))
        weights = jnp.concatenate(weights, axis=0)
        blocks = jnp.concatenate(blocks, axis=0)
        summed = dot(weights, blocks, 0, 0)
        lane_h = iota((pair_rows, LANES), 1) // PER_HEAD_DIM
        parts = []
        for c in range(per):
            for g in range(groups):
                at = (b - g) % groups * slot
                part = summed[at:at + pair_rows, c * LANES:(c + 1) * LANES]
                for h in range(1, heads_per):
                    row = at + h * pair_rows
                    part = jnp.where(
                        lane_h == h,
                        summed[row:row + pair_rows, c * LANES:(c + 1) * LANES], part)
                parts.append(part)
        mixed.append(jnp.concatenate(parts, axis=0))
    attended = jnp.concatenate(mixed, axis=1).astype(BF16)
    gated = (gate_buf[...] * attended.astype(F32)).astype(BF16)
    final_load.wait()
    lr_load.wait()
    updated = (embedding + dot(gated, final_ref[...])).astype(BF16)
    normed_out = layer_normalize(updated).astype(BF16)
    sides_w = jnp.concatenate(
        [lr_ref[:PROJ_FEATURES, :]] * aminos + [lr_ref[PROJ_FEATURES:, :]] * aminos, axis=0)
    sides = dot(normed_out, sides_w, 1, 1)
    two = (rows, 2 * LANES)
    sides = (sides * jnp.concatenate([mask_buf[...]] * 2, axis=1)).astype(BF16)
    sides = jnp.where(iota(two, 1) // PROJ_FEATURES % aminos == iota(two, 0) % aminos,
                      sides, jnp.zeros_like(sides))
    sq = (chains, rows)
    gather = one_hot((iota(sq, 0) // per == iota(sq, 1) % full // aminos)
                     & (iota(sq, 0) % per == iota(sq, 1) // full))
    sides = dot(gather, sides).reshape(ranks, per, 2 * LANES).astype(BF16)
    left = sides[:, :, :LANES].reshape(groups, quads, per, LANES)
    right = sides[:, :, LANES:]
    for r in range(ranks):
        side_send[:, r, :quads] = left
    for g in range(groups):
        side_send[g, :, quads] = right
    for _, g, r in others:
        send(side_send.at[g, r], side_buf.at[:, me], side_r, g, r)
    out_send[...] = updated.astype(F32).reshape(per, ranks, aminos, ROW_FEATURES).astype(BF16)
    for k, g, r in others:
        if k < ranks:
            send(out_send.at[:, r], out_ref.at[own], out_r, g, r)
    side_buf[:, pl.ds(me, 1)] = side_send[group, rank][:, None]
    out_ref[own] = out_send[:, pl.ds(rank, 1)].reshape(per, aminos, ROW_FEATURES)

    at = (pairs, full)
    row_pick = iota(at, 1) == group * pair_rows + iota(at, 0) // aminos
    col_pick = iota(at, 1) == rank * aminos + iota(at, 0) % aminos
    both = jnp.zeros((pairs, LANES), F32)
    for seen in (near_aux[:, LANES:], far_aux[:, LANES:]):
        both = both + dot(one_hot(row_pick), seen) * dot(one_hot(col_pick), seen)
    counts = jnp.sum(both, axis=1, keepdims=True)
    resolved_load.wait()
    resolved = jnp.broadcast_to(resolved_ref[...].astype(F32), at)
    scale = jnp.sum(jnp.where(row_pick, resolved, 0.0), axis=1, keepdims=True) * jnp.sum(
        jnp.where(col_pick, resolved, 0.0), axis=1, keepdims=True) / counts
    scale = jnp.broadcast_to(scale, (pairs, LANES))
    take(outer_ref, load_s.at[8])
    block = iota((pair_rows, LANES), 1) // PROJ_FEATURES
    take(side_all, side_r)
    right_rows = flat(side_buf[quads])
    for q in range(quads):
        product_buf[q * LANES:(q + 1) * LANES, :] = dot(flat(side_buf[q]), right_rows, 0, 0)
    parts = []
    for c in range(PROJ_FEATURES):
        slab = product_buf[pl.ds(c, pair_rows, stride=PROJ_FEATURES), :].astype(BF16)
        parts.append(jnp.concatenate(
            [jnp.where(block == j, slab, jnp.zeros_like(slab)) for j in range(aminos)], axis=0))
    outer = dot(jnp.concatenate(parts, axis=1), flat(outer_ref[...].reshape(-1, CZ)))
    for j in range(aminos):
        turn_buf[pl.ds(j, pair_rows, stride=aminos), :] = outer[j * pair_rows:(j + 1) * pair_rows]
    result = pair_value + scale * turn_buf[...]
    pair_out_ref[...] = result.reshape(pair_rows, aminos, CZ).astype(BF16)
    take(out_all, out_r)
    for view in (near_all, far, side_all, out_all):
        take(view, send_s)


def write_kernel(out_ref, pair_ref, out_hbm, pair_hbm, sem):
    copies = [pltpu.make_async_copy(out_ref, out_hbm, sem.at[0]),
              pltpu.make_async_copy(pair_ref, pair_hbm, sem.at[1])]
    for copy in copies:
        copy.start()
    for copy in copies:
        copy.wait()


def fused(*args):
    emb, mask, resolved, pair = args[:4]
    groups, ranks = lax.axis_size("seq"), lax.axis_size("res")
    chains, aminos = emb.shape[:2]
    per = chains // ranks
    pair_rows = pair.shape[0]
    quads = pair_rows // aminos
    devices = groups * ranks
    operands = (emb.reshape(ranks, per, aminos, ROW_FEATURES), mask.T, resolved.reshape(1, -1), pair, args[4], args[5].T, args[6],
                args[7].T, args[8].reshape(PROJ_FEATURES, PROJ_FEATURES, CZ))
    vmem = pl.BlockSpec(memory_space=pltpu.VMEM)
    whole = pl.BlockSpec(memory_space=pl.ANY)
    dma = pltpu.SemaphoreType.DMA
    results = pl.pallas_call(
        functools.partial(fused_kernel, groups, ranks, per, aminos),
        out_shape=(pltpu.VMEM(emb.shape, BF16), pltpu.VMEM(pair.shape, BF16)),
        in_specs=[whole] * len(operands),
        out_specs=(vmem, vmem),
        scratch_shapes=[
            pltpu.VMEM((ranks, per + 1, aminos, ROW_FEATURES), BF16),
            pltpu.VMEM((per + 1, ranks, aminos, ROW_FEATURES), BF16),
            pltpu.VMEM((ranks, aminos, ROW_FEATURES), BF16),
        ] + [pltpu.VMEM(x.shape, x.dtype) for x in operands[1:8]] + [
            pltpu.VMEM((PROJ_FEATURES, aminos, PROJ_FEATURES, CZ), BF16),
            pltpu.VMEM((groups, ranks, quads + 1, per, LANES), BF16),
            pltpu.VMEM((quads + 1, devices, per, LANES), BF16),
            pltpu.VMEM((per, ranks, aminos, ROW_FEATURES), BF16),
            pltpu.VMEM((chains * aminos, ROW_FEATURES), F32),
            pltpu.VMEM((chains * aminos, LANES), F32),
            pltpu.VMEM((chains * aminos, ROW_FEATURES), F32),
            pltpu.VMEM((chains * aminos, ROW_FEATURES), BF16),
            pltpu.VMEM((pair_rows * PROJ_FEATURES, LANES), F32),
            pltpu.VMEM((pair_rows * aminos, CZ), F32),
            dma((len(operands),)), dma, dma, dma, dma, dma,
        ],
        compiler_params=pltpu.CompilerParams(collective_id=0, has_side_effects=True),
    )(*operands)
    return pl.pallas_call(
        write_kernel,
        out_shape=(jax.ShapeDtypeStruct(emb.shape, BF16), jax.ShapeDtypeStruct(pair.shape, BF16)),
        in_specs=[whole, whole],
        out_specs=(whole, whole),
        scratch_shapes=[dma((2,))],
    )(*[pltpu.with_memory_space_constraint(x, pltpu.VMEM) for x in results])


def fits(mesh, emb, pair):
    groups, ranks = mesh.shape["seq"], mesh.shape["res"]
    chains, aminos = emb.shape[:2]
    if chains % ranks or aminos * PROJ_FEATURES != LANES or chains * aminos != LANES:
        return False
    if ranks & (ranks - 1) or HEAD_NUMBER * PER_HEAD_DIM != groups * LANES:
        return False
    pairs = pair.shape[0] * aminos
    return pairs * groups == LANES and chains // ranks * aminos * groups == PROJ_FEATURES


def solution(mesh):
    placed = (
        P(("crop", "seq"), "res", None),
        P(("crop", "seq"), "res"),
        P("crop"),
        P(("crop", "seq"), "res", None),
        P(),
        P(),
        P(),
        P(),
        P(),
    )
    def either(*args):
        return (fused if fits(mesh, args[0], args[3]) else per_device)(*args)

    return jax.shard_map(
        either,
        mesh=mesh,
        in_specs=placed,
        out_specs=(P(("crop", "seq"), "res", None), P(("crop", "seq"), "res", None)),
        check_vma=False,
    )
```

```python
import functools
import math

import jax
import jax.numpy as jnp
from jax import lax
from jax.experimental import pallas as pl
from jax.experimental.pallas import tpu as pltpu
from jax.sharding import PartitionSpec as P

ROW_FEATURES = 256
CZ = 128
HEAD_NUMBER = 8
PER_HEAD_DIM = 32
PROJ_FEATURES = 32


epsilon = 1e-05


def layer_normalize(values):
    values = values.astype(jnp.float32)
    average = jnp.mean(values, axis=-1, keepdims=True)
    centered = values - average
    variance = jnp.mean(centered * centered, axis=-1, keepdims=True)
    return centered * lax.rsqrt(variance + epsilon)


def outer_rows(left_side, right_side, project):
    row_total = left_side.shape[1]
    col_total = right_side.shape[1]
    block_rows = math.gcd(row_total, max(1, 2048 // col_total))

    def outer_block(start):
        product = jnp.einsum(
            "sic,sje->ijce", left_side, right_side, preferred_element_type=jnp.float32
        )
        flattened = product.reshape(block_rows * col_total, PROJ_FEATURES * PROJ_FEATURES)
        return jnp.dot(flattened, project, precision=lax.Precision.HIGHEST).reshape(
            block_rows, col_total, CZ
        )

    starts = jnp.arange(row_total // block_rows, dtype=jnp.int32) * block_rows
    return lax.map(outer_block, starts).reshape(row_total, col_total, CZ)


def per_device(
    aligned_chain_embedding,
    alignment_mask,
    resolved_residue_mask,
    pairwise_state,
    combined_projection_matrix,
    pair_bias_weight,
    final_projection_matrix,
    left_right_projection_matrix,
    outer_mean_weight,
):
    chain_count = aligned_chain_embedding.shape[0]
    amino_count = aligned_chain_embedding.shape[1]
    res_ranks = lax.axis_size("res")
    seq_groups = lax.axis_size("seq")
    full_length = amino_count * res_ranks
    row_count = full_length // seq_groups
    item_count = HEAD_NUMBER * chain_count // res_ranks
    per_head = min(item_count, chain_count)
    head_count = item_count // per_head
    my_rank = lax.axis_index("res")
    my_group = lax.axis_index("seq")
    standardized_rows = layer_normalize(aligned_chain_embedding).astype(jnp.bfloat16)
    linear_mapped = jnp.dot(
        standardized_rows.reshape(chain_count * amino_count, ROW_FEATURES),
        combined_projection_matrix,
        preferred_element_type=jnp.float32,
    )
    linear_mapped = linear_mapped.reshape(chain_count, amino_count, 4, HEAD_NUMBER, PER_HEAD_DIM)
    queries = (linear_mapped[:, :, 0] * PER_HEAD_DIM ** (-0.5)).astype(jnp.bfloat16)
    key_rows = linear_mapped[:, :, 1].astype(jnp.bfloat16)
    value_rows = linear_mapped[:, :, 2].astype(jnp.bfloat16)
    sigmoid_factor = jax.nn.sigmoid(linear_mapped[:, :, 3])
    stacked = jnp.stack([queries, key_rows, value_rows], axis=2)
    stacked = jnp.transpose(stacked, (3, 0, 1, 2, 4)).reshape(
        HEAD_NUMBER * chain_count, amino_count, 3 * PER_HEAD_DIM
    )
    presence_mask_flags = alignment_mask.astype(jnp.bfloat16)
    key_flags = jnp.broadcast_to(
        presence_mask_flags[None], (HEAD_NUMBER, chain_count, amino_count)
    ).reshape(HEAD_NUMBER * chain_count, amino_count)
    arrived, arrived_flags = (
        lax.all_to_all(stacked, "res", split_axis=0, concat_axis=1, tiled=True),
        lax.all_to_all(key_flags, "res", split_axis=0, concat_axis=1, tiled=True),
    )
    pair_normed = layer_normalize(pairwise_state).astype(jnp.bfloat16)
    local_bias = jnp.dot(
        pair_normed.reshape(row_count * amino_count, CZ),
        pair_bias_weight,
        preferred_element_type=jnp.float32,
    )
    local_bias = jnp.transpose(
        local_bias.astype(jnp.bfloat16).reshape(row_count, amino_count, HEAD_NUMBER), (2, 0, 1)
    )
    bias_cols = lax.all_gather(local_bias, "res", axis=2, tiled=True)
    whole_bias = lax.all_gather(bias_cols, "seq", axis=1, tiled=True)
    first_head = my_rank * item_count // chain_count
    head_bias = lax.dynamic_slice_in_dim(whole_bias, first_head, head_count, 0)
    grouped = arrived.reshape(head_count, per_head, full_length, 3, PER_HEAD_DIM)
    key_validity_mask = (
        arrived_flags.reshape(head_count, per_head, full_length).astype(jnp.float32) - 1.0
    ) * 1000000000.0
    scores = jnp.einsum(
        "gpid,gpjd->gpij",
        grouped[:, :, :, 0],
        grouped[:, :, :, 1],
        preferred_element_type=jnp.float32,
    )
    scores = scores + head_bias.astype(jnp.float32)[:, None] + key_validity_mask[:, :, None, :]
    row_max = jnp.max(scores, axis=-1, keepdims=True)
    exponent = jnp.exp(scores - row_max)
    weights = (exponent / jnp.sum(exponent, axis=-1, keepdims=True)).astype(jnp.bfloat16)
    softmax_mixed = jnp.einsum(
        "gpij,gpjd->gpid", weights, grouped[:, :, :, 2], preferred_element_type=jnp.float32
    )
    softmax_mixed = softmax_mixed.astype(jnp.bfloat16).reshape(
        item_count, full_length, PER_HEAD_DIM
    )
    returned = lax.all_to_all(softmax_mixed, "res", split_axis=1, concat_axis=0, tiled=True)
    returned = jnp.transpose(
        returned.reshape(HEAD_NUMBER, chain_count, amino_count, PER_HEAD_DIM), (1, 2, 0, 3)
    )
    sigmoid_scaled = (
        (sigmoid_factor * returned.astype(jnp.float32))
        .astype(jnp.bfloat16)
        .reshape(chain_count * amino_count, ROW_FEATURES)
    )
    embedding_increment = jnp.dot(
        sigmoid_scaled, final_projection_matrix, preferred_element_type=jnp.float32
    ).reshape(chain_count, amino_count, ROW_FEATURES)
    alignment_output = (aligned_chain_embedding.astype(jnp.float32) + embedding_increment).astype(
        jnp.bfloat16
    )
    standardized_product = layer_normalize(alignment_output).astype(jnp.bfloat16)
    left_right_vectors = jnp.dot(
        standardized_product.reshape(chain_count * amino_count, ROW_FEATURES),
        left_right_projection_matrix,
        preferred_element_type=jnp.float32,
    )
    left_right_vectors = left_right_vectors.reshape(chain_count, amino_count, 2, PROJ_FEATURES)
    entry_present = alignment_mask.astype(jnp.float32)[:, :, None]
    left_side = (left_right_vectors[:, :, 0] * entry_present).astype(jnp.bfloat16)
    right_side = (left_right_vectors[:, :, 1] * entry_present).astype(jnp.bfloat16)
    left_all, left_flags = (
        lax.all_gather(left_side, "res", axis=1, tiled=True),
        lax.all_gather(presence_mask_flags, "res", axis=1, tiled=True),
    )
    project = outer_mean_weight.astype(jnp.float32)
    row_start = my_group * row_count
    left_full, flag_full = (
        lax.all_to_all(left_all, "seq", split_axis=1, concat_axis=0, tiled=True),
        lax.all_to_all(left_flags, "seq", split_axis=1, concat_axis=0, tiled=True),
    )
    right_full, right_flags = (
        lax.all_gather(right_side, "seq", axis=0, tiled=True),
        lax.all_gather(presence_mask_flags, "seq", axis=0, tiled=True),
    )
    counts = jnp.dot(flag_full.T, right_flags, preferred_element_type=jnp.float32)
    outer = outer_rows(left_full, right_full, project)
    col_start = my_rank * amino_count
    row_mask = lax.dynamic_slice_in_dim(resolved_residue_mask, row_start, row_count).astype(
        jnp.float32
    )
    col_mask = lax.dynamic_slice_in_dim(resolved_residue_mask, col_start, amino_count).astype(
        jnp.float32
    )
    pair_mask = row_mask[:, None] * col_mask[None, :]
    pairwise_output = (
        pairwise_state.astype(jnp.float32) + pair_mask[:, :, None] * (outer / counts[:, :, None])
    ).astype(jnp.bfloat16)
    return (alignment_output, pairwise_output)


LANES = 128
F32 = jnp.float32
BF16 = jnp.bfloat16


def iota(shape, axis):
    return lax.broadcasted_iota(jnp.int32, shape, axis)


def dot(a, b, ca=1, cb=0):
    return lax.dot_general(a, b, (((ca,), (cb,)), ((), ())), preferred_element_type=F32)


def one_hot(cond):
    return jnp.where(cond, 1.0, 0.0).astype(BF16)


def flat(block):
    return block.reshape(-1, block.shape[-1])


def turn_blocks(slabs):
    count = len(slabs)
    size = LANES // count
    lane = iota(slabs[0].shape, 1) // size
    slabs = list(slabs)
    half = count // 2
    while half:
        low = lane // half % 2 == 0
        for x in range(count):
            if x // half % 2 == 0:
                a, b = slabs[x], slabs[x + half]
                slabs[x] = jnp.where(low, a, pltpu.roll(b, half * size, 1))
                slabs[x + half] = jnp.where(low, pltpu.roll(a, LANES - half * size, 1), b)
        half //= 2
    return slabs


def fused_kernel(
    groups, ranks, per, aminos,
    emb_hbm, mask_hbm, resolved_hbm, pair_hbm, proj_hbm, bias_hbm, final_hbm, lr_hbm, outer_hbm,
    out_ref, pair_out_ref,
    pack, near, far, mask_ref, resolved_ref, pair_ref, proj_ref, bias_w_ref, final_ref, lr_ref,
    outer_ref, side_send, side_buf, out_send, raw_buf, mask_buf, keep_buf, gate_buf, value_buf,
    pick_ref, gather_ref, sides_w_ref, turn_buf, load_s, send_s, near_r, far_r, side_r, out_r,
):
    devices = groups * ranks
    chains = per * ranks
    full = ranks * aminos
    rows = per * full
    pair_rows = full // groups
    pairs = pair_rows * aminos
    quads = pair_rows // aminos
    width = HEAD_NUMBER * PER_HEAD_DIM
    halves = width // LANES
    heads_per = LANES // PER_HEAD_DIM
    slot = LANES // groups
    folds = 8 // aminos
    cores = math.gcd(2, ranks)
    group = lax.axis_index("seq")
    rank = lax.axis_index("res")
    me = group * ranks + rank

    def flip(k):
        peer = 0
        for bit in range(ranks.bit_length() - 1):
            digit = rank // (1 << bit) % 2
            peer = peer + (1 << bit) * (1 - digit if k >> bit & 1 else digit)
        return peer

    others = []
    for shift in range(groups - 1, -1, -1):
        for k in range(ranks - 1, -1, -1):
            if shift or k:
                others.append((shift * ranks + k, lax.rem(group + shift, groups), flip(k)))

    barrier = pltpu.get_barrier_semaphore()
    for _, g, r in others:
        pl.semaphore_signal(
            barrier, inc=1, device_id={"seq": g, "res": r}, device_id_type=pl.DeviceIdType.MESH
        )

    def load(k, src, dst):
        copy = pltpu.make_async_copy(src, dst, load_s.at[k])
        copy.start()
        return copy

    emb_load = load(0, emb_hbm, pack.at[:, pl.ds(0, per)])
    pair_load = load(1, pair_hbm, pair_ref)
    bias_load = load(2, bias_hbm, bias_w_ref)
    mask_load = load(3, mask_hbm, mask_ref)
    proj_load = load(4, proj_hbm, proj_ref)
    final_load = load(5, final_hbm, final_ref)
    lr_load = load(6, lr_hbm, lr_ref)
    resolved_load = load(7, resolved_hbm, resolved_ref)
    for x in range(folds):
        load(8, outer_hbm.at[:, x], outer_ref.at[:, :, pl.ds(x * CZ, CZ)])

    def send(src, dst, rsem, g, r):
        pltpu.make_async_remote_copy(
            src_ref=src, dst_ref=dst, send_sem=send_s, recv_sem=rsem,
            device_id={"seq": g, "res": r}, device_id_type=pl.DeviceIdType.MESH,
        ).start()

    def take(view, sem):
        pltpu.make_async_copy(view, view, sem).wait()

    own = pl.ds(rank * per, per)
    near_all = near.at[:, pl.ds(0, ranks - 1)]
    side_all = side_buf.at[:, pl.ds(0, devices - 1)]
    out_all = out_ref.at[pl.ds(0, per * (ranks - 1))]

    bias_load.wait()
    lane_head = iota((LANES, HEAD_NUMBER), 0)
    lane_head = (lane_head // slot + group) % groups * heads_per + lane_head % slot // pair_rows
    wide_w = dot(one_hot(lane_head == iota((LANES, HEAD_NUMBER), 1)), bias_w_ref[...]).astype(BF16)
    mask_load.wait()
    flags = dot(mask_ref[...].astype(F32).astype(BF16), one_hot(
        iota((chains, LANES), 0) == iota((chains, LANES), 1)))
    pair_load.wait()
    pair_value = flat(pair_ref[...].astype(F32))
    own_bias = dot(layer_normalize(pair_value).astype(BF16), wide_w, 1, 1)
    own_bias = jnp.where(
        iota((pairs, LANES), 0) // aminos == iota((pairs, LANES), 1) % pair_rows, own_bias, 0.0)
    own_bias = jnp.sum(own_bias.reshape(pair_rows, aminos, LANES), axis=0)
    aux = jnp.concatenate([own_bias, flags], axis=1).astype(BF16)
    for r in range(ranks):
        pack[r, per] = aux
    emb_load.wait()
    near[:, pl.ds(rank, 1)] = pack[rank][:, None]

    pl.semaphore_wait(barrier, devices - 1)
    for k, g, r in others:
        if k < ranks:
            send(pack.at[r], near.at[:, rank], near_r, g, r)
        else:
            send(pack.at[0, per], far.at[rank], far_r, g, r)

    for copy in (proj_load, final_load, lr_load, resolved_load):
        copy.wait()
    block_mask = (iota((LANES, LANES), 0) % slot // pair_rows
                  == iota((LANES, LANES), 1) // PER_HEAD_DIM)
    at = (LANES, per * LANES)
    pick_ref[...] = one_hot(iota(at, 0) == rank * per + iota(at, 1) // LANES)
    at = (chains, rows)
    gather_ref[...] = one_hot((iota(at, 0) // per == iota(at, 1) % full // aminos)
                              & (iota(at, 0) % per == iota(at, 1) // full))
    at = (2 * LANES, 2 * PROJ_FEATURES)
    left_row, right_row = iota(at, 0) // aminos, PROJ_FEATURES + iota(at, 0) % PROJ_FEATURES
    sides_w_ref[...] = dot(one_hot(
        jnp.where(iota(at, 0) < LANES, left_row, right_row) == iota(at, 1)), lr_ref[...]).astype(BF16)
    two = (rows, 2 * LANES)
    amino = jnp.where(iota(two, 1) < LANES, iota(two, 1) % aminos,
                      iota(two, 1) % LANES // PROJ_FEATURES)
    keep_buf[...] = jnp.where(amino == iota(two, 0) % aminos, 1.0, 0.0)
    take(near_all, near_r)
    embedding = near[:per].astype(F32).reshape(rows, ROW_FEATURES)
    normed = layer_normalize(embedding).astype(BF16)
    projected = dot(normed, proj_ref[...])
    queries = (projected[:, :width] * PER_HEAD_DIM ** (-0.5)).astype(BF16)
    keys = projected[:, width:2 * width].astype(BF16)
    value_buf[...] = projected[:, 2 * width:3 * width].astype(BF16)
    gate_buf[...] = jax.nn.sigmoid(projected[:, 3 * width:])

    for b in range(halves):
        cols = slice(b * LANES, (b + 1) * LANES)
        for c in range(per):
            spread = []
            for s in range(groups):
                at = c * full + (b - s) % groups * pair_rows
                spread += [queries[at:at + pair_rows, cols]] * heads_per
            spread = jnp.concatenate(spread, axis=0)
            spread = jnp.where(block_mask, spread, jnp.zeros_like(spread))
            raw_buf[c * full:(c + 1) * full, cols] = dot(
                keys[c * full:(c + 1) * full, cols], spread, 1, 1)

    near_aux = flat(near[per])
    key_flags = dot(near_aux[:, LANES:], pick_ref[...])
    for c in range(per):
        at = slice(c * full, (c + 1) * full)
        present = key_flags[:, c * LANES:(c + 1) * LANES]
        mask_buf[at, :] = (present - 1.0) * 1000000000.0
        keep_buf[at, :] = keep_buf[at, :] * jnp.concatenate([present] * 2, axis=1)
    take(far, far_r)
    far_aux = flat(far[...])
    near_bias = near_aux[:, :LANES].astype(F32)
    far_bias = far_aux[:, :LANES].astype(F32)
    which = iota((full, LANES), 1) // slot
    mixed = []
    for b in range(halves):
        cols = slice(b * LANES, (b + 1) * LANES)
        tile_bias = jnp.where((b + which) % groups == group, near_bias, far_bias)
        weights, blocks = [], []
        for c in range(per):
            at = slice(c * full, (c + 1) * full)
            scores = raw_buf[at, cols] + tile_bias + mask_buf[at, :]
            exponent = jnp.exp(scores - jnp.max(scores, axis=0, keepdims=True))
            total = 1.0 / jnp.sum(exponent, axis=0, keepdims=True)
            weights.append((exponent * total).astype(BF16))
            own_values = value_buf[at, cols]
            blocks.append(jnp.concatenate(
                [own_values if d == c else jnp.zeros_like(own_values) for d in range(per)], axis=1))
        weights = jnp.concatenate(weights, axis=0)
        blocks = jnp.concatenate(blocks, axis=0)
        summed = dot(weights, blocks, 0, 0)
        lane_h = iota((pair_rows, LANES), 1) // PER_HEAD_DIM
        parts = []
        for c in range(per):
            for g in range(groups):
                at = (b - g) % groups * slot
                part = summed[at:at + pair_rows, c * LANES:(c + 1) * LANES]
                for h in range(1, heads_per):
                    row = at + h * pair_rows
                    part = jnp.where(
                        lane_h == h,
                        summed[row:row + pair_rows, c * LANES:(c + 1) * LANES], part)
                parts.append(part)
        mixed.append(jnp.concatenate(parts, axis=0))
    attended = jnp.concatenate(mixed, axis=1).astype(BF16)
    gated = (gate_buf[...] * attended.astype(F32)).astype(BF16)
    updated = (embedding + dot(gated, final_ref[...])).astype(BF16)
    out_send[...] = updated.astype(F32).reshape(per, ranks, aminos, ROW_FEATURES).astype(BF16)
    normed_out = layer_normalize(updated).astype(BF16)
    sides = (dot(normed_out, sides_w_ref[...], 1, 1) * keep_buf[...]).astype(BF16)
    sides = dot(gather_ref[...], sides).reshape(ranks, per, 2 * LANES).astype(BF16)
    left = sides[:, :, :LANES].reshape(groups, quads, per, LANES)
    right = sides[:, :, LANES:]
    for r in range(ranks):
        side_send[:, r, :quads] = left
    for g in range(groups):
        side_send[g, :, quads] = right
    place = rank // cores * groups * cores + group * cores + lax.rem(rank, cores)
    for n in range(devices - 1):
        at = n + lax.div(n - place + devices, devices)
        g = lax.rem(lax.div(at, cores), groups)
        r = lax.div(at, groups * cores) * cores + lax.rem(at, cores)
        send(side_send.at[g, r], side_buf.at[:, me], side_r, g, r)
        if n % (groups * cores) == cores - 1:
            for m in range(n // groups // cores * cores, n // groups // cores * cores + cores):
                if m < ranks - 1:
                    r = m + lax.div(m - rank + ranks, ranks)
                    send(out_send.at[:, r], out_ref.at[own], out_r, group, r)
    side_buf[:, pl.ds(me, 1)] = side_send[group, rank][:, None]
    out_ref[own] = out_send[:, pl.ds(rank, 1)].reshape(per, aminos, ROW_FEATURES)

    at = (pairs, full)
    row_pick = iota(at, 1) == group * pair_rows + iota(at, 0) // aminos
    col_pick = iota(at, 1) == rank * aminos + iota(at, 0) % aminos
    both = jnp.zeros((pairs, LANES), F32)
    for seen in (near_aux[:, LANES:], far_aux[:, LANES:]):
        both = both + dot(one_hot(row_pick), seen) * dot(one_hot(col_pick), seen)
    counts = jnp.sum(both, axis=1, keepdims=True)
    resolved = jnp.broadcast_to(resolved_ref[...].astype(F32), at)
    scale = jnp.sum(jnp.where(row_pick, resolved, 0.0), axis=1, keepdims=True) * jnp.sum(
        jnp.where(col_pick, resolved, 0.0), axis=1, keepdims=True) / counts
    scale = jnp.broadcast_to(scale, (pairs, LANES))
    take(outer_ref, load_s.at[8])
    take(side_all, side_r)
    right_rows = flat(side_buf[quads])
    products = [dot(flat(side_buf[q]), right_rows, 0, 0) for q in range(quads)]
    parts = []
    step = folds * aminos
    for c in range(0, PROJ_FEATURES // folds, aminos):
        slabs = []
        for x in range(c, c + aminos):
            slab = [product[x * step:(x + 1) * step] for product in products]
            slabs.append(jnp.concatenate(slab, axis=0))
        parts.append(jnp.concatenate(turn_blocks(slabs), axis=0).astype(BF16))
    outer = dot(jnp.concatenate(parts, axis=1), outer_ref[...].reshape(-1, folds * CZ))
    for j in range(aminos):
        for q in range(quads):
            base = (j * quads + q) * folds * aminos
            total = outer[base:base + aminos, :CZ]
            for x in range(1, folds):
                row = base + x * aminos
                total = total + outer[row:row + aminos, x * CZ:(x + 1) * CZ]
            turn_buf[pl.ds(q * aminos * aminos + j, aminos, stride=aminos), :] = total
    result = pair_value + scale * turn_buf[...]
    pair_out_ref[...] = result.reshape(pair_rows, aminos, CZ).astype(BF16)
    take(out_all, out_r)
    for view in (near_all, far, side_all, out_all):
        take(view, send_s)


def write_kernel(out_ref, pair_ref, out_hbm, pair_hbm, sem):
    copies = [pltpu.make_async_copy(out_ref, out_hbm, sem.at[0]),
              pltpu.make_async_copy(pair_ref, pair_hbm, sem.at[1])]
    for copy in copies:
        copy.start()
    for copy in copies:
        copy.wait()


def fused(*args):
    emb, mask, resolved, pair = args[:4]
    groups, ranks = lax.axis_size("seq"), lax.axis_size("res")
    chains, aminos = emb.shape[:2]
    per = chains // ranks
    pair_rows = pair.shape[0]
    quads = pair_rows // aminos
    devices = groups * ranks
    folds = 8 // aminos
    operands = (emb.reshape(ranks, per, aminos, ROW_FEATURES), mask.T, resolved.reshape(1, -1), pair, args[4], args[5].T, args[6],
                args[7].T, args[8].reshape(PROJ_FEATURES // folds, folds, PROJ_FEATURES, CZ))
    vmem = pl.BlockSpec(memory_space=pltpu.VMEM)
    whole = pl.BlockSpec(memory_space=pl.ANY)
    dma = pltpu.SemaphoreType.DMA
    results = pl.pallas_call(
        functools.partial(fused_kernel, groups, ranks, per, aminos),
        out_shape=(pltpu.VMEM(emb.shape, BF16), pltpu.VMEM(pair.shape, BF16)),
        in_specs=[whole] * len(operands),
        out_specs=(vmem, vmem),
        scratch_shapes=[
            pltpu.VMEM((ranks, per + 1, aminos, ROW_FEATURES), BF16),
            pltpu.VMEM((per + 1, ranks, aminos, ROW_FEATURES), BF16),
            pltpu.VMEM((ranks, aminos, ROW_FEATURES), BF16),
        ] + [pltpu.VMEM(x.shape, x.dtype) for x in operands[1:8]] + [
            pltpu.VMEM((PROJ_FEATURES // folds, PROJ_FEATURES, folds * CZ), BF16),
            pltpu.VMEM((groups, ranks, quads + 1, per, LANES), BF16),
            pltpu.VMEM((quads + 1, devices, per, LANES), BF16),
            pltpu.VMEM((per, ranks, aminos, ROW_FEATURES), BF16),
            pltpu.VMEM((chains * aminos, ROW_FEATURES), F32),
            pltpu.VMEM((chains * aminos, LANES), F32),
            pltpu.VMEM((chains * aminos, 2 * LANES), F32),
            pltpu.VMEM((chains * aminos, ROW_FEATURES), F32),
            pltpu.VMEM((chains * aminos, ROW_FEATURES), BF16),
            pltpu.VMEM((LANES, per * LANES), BF16),
            pltpu.VMEM((chains, chains * aminos), BF16),
            pltpu.VMEM((2 * LANES, ROW_FEATURES), BF16),
            pltpu.VMEM((pair_rows * aminos, CZ), F32),
            dma((len(operands),)), dma, dma, dma, dma, dma,
        ],
        compiler_params=pltpu.CompilerParams(collective_id=0, has_side_effects=True),
    )(*operands)
    return pl.pallas_call(
        write_kernel,
        out_shape=(jax.ShapeDtypeStruct(emb.shape, BF16), jax.ShapeDtypeStruct(pair.shape, BF16)),
        in_specs=[whole, whole],
        out_specs=(whole, whole),
        scratch_shapes=[dma((2,))],
    )(*[pltpu.with_memory_space_constraint(x, pltpu.VMEM) for x in results])


def fits(mesh, emb, pair):
    groups, ranks = mesh.shape["seq"], mesh.shape["res"]
    chains, aminos = emb.shape[:2]
    if chains % ranks or aminos * PROJ_FEATURES != LANES or chains * aminos != LANES:
        return False
    if ranks & (ranks - 1) or HEAD_NUMBER * PER_HEAD_DIM != groups * LANES:
        return False
    pairs = pair.shape[0] * aminos
    return pairs * groups == LANES and chains // ranks * aminos * groups == PROJ_FEATURES


def solution(mesh):
    placed = (
        P(("crop", "seq"), "res", None),
        P(("crop", "seq"), "res"),
        P("crop"),
        P(("crop", "seq"), "res", None),
        P(),
        P(),
        P(),
        P(),
        P(),
    )
    def either(*args):
        return (fused if fits(mesh, args[0], args[3]) else per_device)(*args)

    return jax.shard_map(
        either,
        mesh=mesh,
        in_specs=placed,
        out_specs=(P(("crop", "seq"), "res", None), P(("crop", "seq"), "res", None)),
        check_vma=False,
    )
```

```python
import functools
import math

import jax
import jax.numpy as jnp
from jax import lax
from jax.experimental import pallas as pl
from jax.experimental.pallas import tpu as pltpu
from jax.sharding import PartitionSpec as P

ROW_FEATURES = 256
CZ = 128
HEAD_NUMBER = 8
PER_HEAD_DIM = 32
PROJ_FEATURES = 32


epsilon = 1e-05


def layer_normalize(values):
    values = values.astype(jnp.float32)
    average = jnp.mean(values, axis=-1, keepdims=True)
    centered = values - average
    variance = jnp.mean(centered * centered, axis=-1, keepdims=True)
    return centered * lax.rsqrt(variance + epsilon)


def outer_rows(left_side, right_side, project):
    row_total = left_side.shape[1]
    col_total = right_side.shape[1]
    block_rows = math.gcd(row_total, max(1, 2048 // col_total))

    def outer_block(start):
        product = jnp.einsum(
            "sic,sje->ijce", left_side, right_side, preferred_element_type=jnp.float32
        )
        flattened = product.reshape(block_rows * col_total, PROJ_FEATURES * PROJ_FEATURES)
        return jnp.dot(flattened, project, precision=lax.Precision.HIGHEST).reshape(
            block_rows, col_total, CZ
        )

    starts = jnp.arange(row_total // block_rows, dtype=jnp.int32) * block_rows
    return lax.map(outer_block, starts).reshape(row_total, col_total, CZ)


def per_device(
    aligned_chain_embedding,
    alignment_mask,
    resolved_residue_mask,
    pairwise_state,
    combined_projection_matrix,
    pair_bias_weight,
    final_projection_matrix,
    left_right_projection_matrix,
    outer_mean_weight,
):
    chain_count = aligned_chain_embedding.shape[0]
    amino_count = aligned_chain_embedding.shape[1]
    res_ranks = lax.axis_size("res")
    seq_groups = lax.axis_size("seq")
    full_length = amino_count * res_ranks
    row_count = full_length // seq_groups
    item_count = HEAD_NUMBER * chain_count // res_ranks
    per_head = min(item_count, chain_count)
    head_count = item_count // per_head
    my_rank = lax.axis_index("res")
    my_group = lax.axis_index("seq")
    standardized_rows = layer_normalize(aligned_chain_embedding).astype(jnp.bfloat16)
    linear_mapped = jnp.dot(
        standardized_rows.reshape(chain_count * amino_count, ROW_FEATURES),
        combined_projection_matrix,
        preferred_element_type=jnp.float32,
    )
    linear_mapped = linear_mapped.reshape(chain_count, amino_count, 4, HEAD_NUMBER, PER_HEAD_DIM)
    queries = (linear_mapped[:, :, 0] * PER_HEAD_DIM ** (-0.5)).astype(jnp.bfloat16)
    key_rows = linear_mapped[:, :, 1].astype(jnp.bfloat16)
    value_rows = linear_mapped[:, :, 2].astype(jnp.bfloat16)
    sigmoid_factor = jax.nn.sigmoid(linear_mapped[:, :, 3])
    stacked = jnp.stack([queries, key_rows, value_rows], axis=2)
    stacked = jnp.transpose(stacked, (3, 0, 1, 2, 4)).reshape(
        HEAD_NUMBER * chain_count, amino_count, 3 * PER_HEAD_DIM
    )
    presence_mask_flags = alignment_mask.astype(jnp.bfloat16)
    key_flags = jnp.broadcast_to(
        presence_mask_flags[None], (HEAD_NUMBER, chain_count, amino_count)
    ).reshape(HEAD_NUMBER * chain_count, amino_count)
    arrived, arrived_flags = (
        lax.all_to_all(stacked, "res", split_axis=0, concat_axis=1, tiled=True),
        lax.all_to_all(key_flags, "res", split_axis=0, concat_axis=1, tiled=True),
    )
    pair_normed = layer_normalize(pairwise_state).astype(jnp.bfloat16)
    local_bias = jnp.dot(
        pair_normed.reshape(row_count * amino_count, CZ),
        pair_bias_weight,
        preferred_element_type=jnp.float32,
    )
    local_bias = jnp.transpose(
        local_bias.astype(jnp.bfloat16).reshape(row_count, amino_count, HEAD_NUMBER), (2, 0, 1)
    )
    bias_cols = lax.all_gather(local_bias, "res", axis=2, tiled=True)
    whole_bias = lax.all_gather(bias_cols, "seq", axis=1, tiled=True)
    first_head = my_rank * item_count // chain_count
    head_bias = lax.dynamic_slice_in_dim(whole_bias, first_head, head_count, 0)
    grouped = arrived.reshape(head_count, per_head, full_length, 3, PER_HEAD_DIM)
    key_validity_mask = (
        arrived_flags.reshape(head_count, per_head, full_length).astype(jnp.float32) - 1.0
    ) * 1000000000.0
    scores = jnp.einsum(
        "gpid,gpjd->gpij",
        grouped[:, :, :, 0],
        grouped[:, :, :, 1],
        preferred_element_type=jnp.float32,
    )
    scores = scores + head_bias.astype(jnp.float32)[:, None] + key_validity_mask[:, :, None, :]
    row_max = jnp.max(scores, axis=-1, keepdims=True)
    exponent = jnp.exp(scores - row_max)
    weights = (exponent / jnp.sum(exponent, axis=-1, keepdims=True)).astype(jnp.bfloat16)
    softmax_mixed = jnp.einsum(
        "gpij,gpjd->gpid", weights, grouped[:, :, :, 2], preferred_element_type=jnp.float32
    )
    softmax_mixed = softmax_mixed.astype(jnp.bfloat16).reshape(
        item_count, full_length, PER_HEAD_DIM
    )
    returned = lax.all_to_all(softmax_mixed, "res", split_axis=1, concat_axis=0, tiled=True)
    returned = jnp.transpose(
        returned.reshape(HEAD_NUMBER, chain_count, amino_count, PER_HEAD_DIM), (1, 2, 0, 3)
    )
    sigmoid_scaled = (
        (sigmoid_factor * returned.astype(jnp.float32))
        .astype(jnp.bfloat16)
        .reshape(chain_count * amino_count, ROW_FEATURES)
    )
    embedding_increment = jnp.dot(
        sigmoid_scaled, final_projection_matrix, preferred_element_type=jnp.float32
    ).reshape(chain_count, amino_count, ROW_FEATURES)
    alignment_output = (aligned_chain_embedding.astype(jnp.float32) + embedding_increment).astype(
        jnp.bfloat16
    )
    standardized_product = layer_normalize(alignment_output).astype(jnp.bfloat16)
    left_right_vectors = jnp.dot(
        standardized_product.reshape(chain_count * amino_count, ROW_FEATURES),
        left_right_projection_matrix,
        preferred_element_type=jnp.float32,
    )
    left_right_vectors = left_right_vectors.reshape(chain_count, amino_count, 2, PROJ_FEATURES)
    entry_present = alignment_mask.astype(jnp.float32)[:, :, None]
    left_side = (left_right_vectors[:, :, 0] * entry_present).astype(jnp.bfloat16)
    right_side = (left_right_vectors[:, :, 1] * entry_present).astype(jnp.bfloat16)
    left_all, left_flags = (
        lax.all_gather(left_side, "res", axis=1, tiled=True),
        lax.all_gather(presence_mask_flags, "res", axis=1, tiled=True),
    )
    project = outer_mean_weight.astype(jnp.float32)
    row_start = my_group * row_count
    left_full, flag_full = (
        lax.all_to_all(left_all, "seq", split_axis=1, concat_axis=0, tiled=True),
        lax.all_to_all(left_flags, "seq", split_axis=1, concat_axis=0, tiled=True),
    )
    right_full, right_flags = (
        lax.all_gather(right_side, "seq", axis=0, tiled=True),
        lax.all_gather(presence_mask_flags, "seq", axis=0, tiled=True),
    )
    counts = jnp.dot(flag_full.T, right_flags, preferred_element_type=jnp.float32)
    outer = outer_rows(left_full, right_full, project)
    col_start = my_rank * amino_count
    row_mask = lax.dynamic_slice_in_dim(resolved_residue_mask, row_start, row_count).astype(
        jnp.float32
    )
    col_mask = lax.dynamic_slice_in_dim(resolved_residue_mask, col_start, amino_count).astype(
        jnp.float32
    )
    pair_mask = row_mask[:, None] * col_mask[None, :]
    pairwise_output = (
        pairwise_state.astype(jnp.float32) + pair_mask[:, :, None] * (outer / counts[:, :, None])
    ).astype(jnp.bfloat16)
    return (alignment_output, pairwise_output)


LANES = 128
F32 = jnp.float32
BF16 = jnp.bfloat16


def iota(shape, axis):
    return lax.broadcasted_iota(jnp.int32, shape, axis)


def dot(a, b, ca=1, cb=0):
    return lax.dot_general(a, b, (((ca,), (cb,)), ((), ())), preferred_element_type=F32)


def one_hot(cond):
    return jnp.where(cond, 1.0, 0.0).astype(BF16)


def flat(block):
    return block.reshape(-1, block.shape[-1])


def turn_blocks(slabs):
    count = len(slabs)
    size = LANES // count
    lane = iota(slabs[0].shape, 1) // size
    slabs = list(slabs)
    half = count // 2
    while half:
        low = lane // half % 2 == 0
        for x in range(count):
            if x // half % 2 == 0:
                a, b = slabs[x], slabs[x + half]
                slabs[x] = jnp.where(low, a, pltpu.roll(b, half * size, 1))
                slabs[x + half] = jnp.where(low, pltpu.roll(a, LANES - half * size, 1), b)
        half //= 2
    return slabs


def fused_kernel(
    groups, ranks, per, aminos,
    emb_hbm, mask_hbm, resolved_hbm, pair_hbm, proj_hbm, bias_hbm, final_hbm, lr_hbm, outer_hbm,
    out_ref, pair_out_ref,
    pack, near, far, mask_ref, resolved_ref, pair_ref, proj_ref, bias_w_ref, final_ref, lr_ref,
    outer_ref, side_send, side_buf, out_send, raw_buf, mask_buf, keep_buf, gate_buf, value_buf,
    pick_ref, gather_ref, sides_w_ref, turn_buf, load_s, send_s, near_r, far_r, side_r, out_r,
):
    devices = groups * ranks
    chains = per * ranks
    full = ranks * aminos
    rows = per * full
    pair_rows = full // groups
    pairs = pair_rows * aminos
    quads = pair_rows // aminos
    width = HEAD_NUMBER * PER_HEAD_DIM
    halves = width // LANES
    heads_per = LANES // PER_HEAD_DIM
    slot = LANES // groups
    folds = 8 // aminos
    cores = math.gcd(2, ranks)
    group = lax.axis_index("seq")
    rank = lax.axis_index("res")
    me = group * ranks + rank

    chip, core = rank // cores, rank % cores

    def flip(k):
        peer = 0
        for bit in range((ranks // cores).bit_length() - 1):
            digit = chip // (1 << bit) % 2
            peer = peer + (1 << bit) * (1 - digit if k >> bit & 1 else digit)
        return peer

    others = []
    for shift in range(groups - 1, -1, -1):
        g = lax.rem(group + shift, groups)
        for k in range(ranks // cores - 1, -1, -1):
            for x in range(cores):
                if shift or k:
                    others.append((shift, g, flip(k) * cores + x))
    for x in range(1, cores):
        others.append((0, group, chip * cores + lax.rem(core + x, cores)))

    barrier = pltpu.get_barrier_semaphore()
    for _, g, r in others:
        pl.semaphore_signal(
            barrier, inc=1, device_id={"seq": g, "res": r}, device_id_type=pl.DeviceIdType.MESH
        )

    def load(k, src, dst):
        copy = pltpu.make_async_copy(src, dst, load_s.at[k])
        copy.start()
        return copy

    emb_load = load(0, emb_hbm, pack.at[:, pl.ds(0, per)])
    pair_load = load(1, pair_hbm, pair_ref)
    bias_load = load(2, bias_hbm, bias_w_ref)
    mask_load = load(3, mask_hbm, mask_ref)
    proj_load = load(4, proj_hbm, proj_ref)
    final_load = load(4, final_hbm, final_ref)
    lr_load = load(4, lr_hbm, lr_ref)
    resolved_load = load(4, resolved_hbm, resolved_ref)
    for x in range(folds):
        load(5, outer_hbm.at[:, x], outer_ref.at[:, :, pl.ds(x * CZ, CZ)])

    def send(src, dst, rsem, g, r):
        pltpu.make_async_remote_copy(
            src_ref=src, dst_ref=dst, send_sem=send_s, recv_sem=rsem,
            device_id={"seq": g, "res": r}, device_id_type=pl.DeviceIdType.MESH,
        ).start()

    def take(view, sem):
        pltpu.make_async_copy(view, view, sem).wait()

    own = pl.ds(rank * per, per)
    near_all = near.at[:, pl.ds(0, ranks - 1)]
    side_all = side_buf.at[:, pl.ds(0, devices - 1)]
    out_all = out_ref.at[pl.ds(0, per * (ranks - 1))]

    bias_load.wait()
    lane_head = iota((LANES, HEAD_NUMBER), 0)
    lane_head = (lane_head // slot + group) % groups * heads_per + lane_head % slot // pair_rows
    wide_w = dot(one_hot(lane_head == iota((LANES, HEAD_NUMBER), 1)), bias_w_ref[...]).astype(BF16)
    mask_load.wait()
    flags = dot(mask_ref[...].astype(F32).astype(BF16), one_hot(
        iota((chains, LANES), 0) == iota((chains, LANES), 1)))
    pair_load.wait()
    pair_value = flat(pair_ref[...].astype(F32))
    own_bias = dot(layer_normalize(pair_value).astype(BF16), wide_w, 1, 1)
    own_bias = jnp.where(
        iota((pairs, LANES), 0) // aminos == iota((pairs, LANES), 1) % pair_rows, own_bias, 0.0)
    own_bias = jnp.sum(own_bias.reshape(pair_rows, aminos, LANES), axis=0)
    aux = jnp.concatenate([own_bias, flags], axis=1).astype(BF16)
    for r in range(ranks):
        pack[r, per] = aux
    emb_load.wait()
    near[:, pl.ds(rank, 1)] = pack[rank][:, None]

    pl.semaphore_wait(barrier, devices - 1)
    for shift, g, r in others:
        if shift:
            send(pack.at[0, per], far.at[rank], far_r, g, r)
        else:
            send(pack.at[r], near.at[:, rank], near_r, g, r)

    for copy in (proj_load, final_load, lr_load, resolved_load):
        copy.wait()
    block_mask = (iota((LANES, LANES), 0) % slot // pair_rows
                  == iota((LANES, LANES), 1) // PER_HEAD_DIM)
    at = (LANES, per * LANES)
    pick_ref[...] = one_hot(iota(at, 0) == rank * per + iota(at, 1) // LANES)
    at = (chains, rows)
    gather_ref[...] = one_hot((iota(at, 0) // per == iota(at, 1) % full // aminos)
                              & (iota(at, 0) % per == iota(at, 1) // full))
    at = (2 * LANES, 2 * PROJ_FEATURES)
    left_row, right_row = iota(at, 0) // aminos, PROJ_FEATURES + iota(at, 0) % PROJ_FEATURES
    sides_w_ref[...] = dot(one_hot(
        jnp.where(iota(at, 0) < LANES, left_row, right_row) == iota(at, 1)), lr_ref[...]).astype(BF16)
    two = (rows, 2 * LANES)
    amino = jnp.where(iota(two, 1) < LANES, iota(two, 1) % aminos,
                      iota(two, 1) % LANES // PROJ_FEATURES)
    keep_buf[...] = jnp.where(amino == iota(two, 0) % aminos, 1.0, 0.0)
    take(near_all, near_r)
    embedding = near[:per].astype(F32).reshape(rows, ROW_FEATURES)
    normed = layer_normalize(embedding).astype(BF16)
    projected = dot(normed, proj_ref[...])
    queries = (projected[:, :width] * PER_HEAD_DIM ** (-0.5)).astype(BF16)
    keys = projected[:, width:2 * width].astype(BF16)
    value_buf[...] = projected[:, 2 * width:3 * width].astype(BF16)
    gate_buf[...] = jax.nn.sigmoid(projected[:, 3 * width:])

    for b in range(halves):
        cols = slice(b * LANES, (b + 1) * LANES)
        for c in range(per):
            spread = []
            for s in range(groups):
                at = c * full + (b - s) % groups * pair_rows
                spread += [queries[at:at + pair_rows, cols]] * heads_per
            spread = jnp.concatenate(spread, axis=0)
            spread = jnp.where(block_mask, spread, jnp.zeros_like(spread))
            raw_buf[c * full:(c + 1) * full, cols] = dot(
                keys[c * full:(c + 1) * full, cols], spread, 1, 1)

    near_aux = flat(near[per])
    key_flags = dot(near_aux[:, LANES:], pick_ref[...])
    for c in range(per):
        at = slice(c * full, (c + 1) * full)
        present = key_flags[:, c * LANES:(c + 1) * LANES]
        mask_buf[at, :] = (present - 1.0) * 1000000000.0
        keep_buf[at, :] = keep_buf[at, :] * jnp.concatenate([present] * 2, axis=1)
    take(far, far_r)
    far_aux = flat(far[...])
    near_bias = near_aux[:, :LANES].astype(F32)
    far_bias = far_aux[:, :LANES].astype(F32)
    which = iota((full, LANES), 1) // slot
    mixed = []
    for b in range(halves):
        cols = slice(b * LANES, (b + 1) * LANES)
        tile_bias = jnp.where((b + which) % groups == group, near_bias, far_bias)
        weights, blocks = [], []
        for c in range(per):
            at = slice(c * full, (c + 1) * full)
            scores = raw_buf[at, cols] + tile_bias + mask_buf[at, :]
            exponent = jnp.exp(scores - jnp.max(scores, axis=0, keepdims=True))
            total = 1.0 / jnp.sum(exponent, axis=0, keepdims=True)
            weights.append((exponent * total).astype(BF16))
            own_values = value_buf[at, cols]
            blocks.append(jnp.concatenate(
                [own_values if d == c else jnp.zeros_like(own_values) for d in range(per)], axis=1))
        weights = jnp.concatenate(weights, axis=0)
        blocks = jnp.concatenate(blocks, axis=0)
        summed = dot(weights, blocks, 0, 0)
        lane_h = iota((pair_rows, LANES), 1) // PER_HEAD_DIM
        parts = []
        for c in range(per):
            for g in range(groups):
                at = (b - g) % groups * slot
                part = summed[at:at + pair_rows, c * LANES:(c + 1) * LANES]
                for h in range(1, heads_per):
                    row = at + h * pair_rows
                    part = jnp.where(
                        lane_h == h,
                        summed[row:row + pair_rows, c * LANES:(c + 1) * LANES], part)
                parts.append(part)
        mixed.append(jnp.concatenate(parts, axis=0))
    attended = jnp.concatenate(mixed, axis=1).astype(BF16)
    gated = (gate_buf[...] * attended.astype(F32)).astype(BF16)
    updated = (embedding + dot(gated, final_ref[...])).astype(BF16)
    out_send[...] = updated.astype(F32).reshape(per, ranks, aminos, ROW_FEATURES).astype(BF16)
    normed_out = layer_normalize(updated).astype(BF16)
    sides = (dot(normed_out, sides_w_ref[...], 1, 1) * keep_buf[...]).astype(BF16)
    sides = dot(gather_ref[...], sides).reshape(ranks, per, 2 * LANES).astype(BF16)
    left = sides[:, :, :LANES].reshape(groups, quads, per, LANES)
    right = sides[:, :, LANES:]
    def fill(start, stop):
        for r in range(start, stop):
            side_send[:, r, :quads] = left
        for g in range(groups):
            side_send[g, start:stop, quads] = right[start:stop]

    fill(0, 2 * cores)
    place = rank // cores * groups * cores + group * cores + lax.rem(rank, cores)
    for n in range(devices - 1):
        at = n + lax.div(n - place + devices, devices)
        g = lax.rem(lax.div(at, cores), groups)
        r = lax.div(at, groups * cores) * cores + lax.rem(at, cores)
        send(side_send.at[g, r], side_buf.at[:, me], side_r, g, r)
        if n == cores - 1:
            fill(2 * cores, ranks)
        if n % (groups * cores) == cores - 1:
            for m in range(n // groups // cores * cores, n // groups // cores * cores + cores):
                if m < ranks - 1:
                    r = m + lax.div(m - rank + ranks, ranks)
                    send(out_send.at[:, r], out_ref.at[own], out_r, group, r)
    side_buf[:, pl.ds(me, 1)] = side_send[group, rank][:, None]
    out_ref[own] = out_send[:, pl.ds(rank, 1)].reshape(per, aminos, ROW_FEATURES)

    at = (pairs, full)
    row_pick = iota(at, 1) == group * pair_rows + iota(at, 0) // aminos
    col_pick = iota(at, 1) == rank * aminos + iota(at, 0) % aminos
    both = jnp.zeros((pairs, LANES), F32)
    for seen in (near_aux[:, LANES:], far_aux[:, LANES:]):
        both = both + dot(one_hot(row_pick), seen) * dot(one_hot(col_pick), seen)
    counts = jnp.sum(both, axis=1, keepdims=True)
    resolved = jnp.broadcast_to(resolved_ref[...].astype(F32), at)
    scale = jnp.sum(jnp.where(row_pick, resolved, 0.0), axis=1, keepdims=True) * jnp.sum(
        jnp.where(col_pick, resolved, 0.0), axis=1, keepdims=True) / counts
    scale = jnp.broadcast_to(scale, (pairs, LANES))
    take(outer_ref, load_s.at[5])
    take(side_all, side_r)
    right_rows = flat(side_buf[quads])
    products = [dot(flat(side_buf[q]), right_rows, 0, 0) for q in range(quads)]
    parts = []
    step = folds * aminos
    for c in range(0, PROJ_FEATURES // folds, aminos):
        slabs = []
        for x in range(c, c + aminos):
            slab = [product[x * step:(x + 1) * step] for product in products]
            slabs.append(jnp.concatenate(slab, axis=0).astype(BF16))
        parts.append(jnp.concatenate(turn_blocks(slabs), axis=0))
    outer = dot(jnp.concatenate(parts, axis=1), outer_ref[...].reshape(-1, folds * CZ))
    for j in range(aminos):
        for q in range(quads):
            base = (j * quads + q) * folds * aminos
            total = outer[base:base + aminos, :CZ]
            for x in range(1, folds):
                row = base + x * aminos
                total = total + outer[row:row + aminos, x * CZ:(x + 1) * CZ]
            turn_buf[pl.ds(q * aminos * aminos + j, aminos, stride=aminos), :] = total
    result = pair_value + scale * turn_buf[...]
    pair_out_ref[...] = result.reshape(pair_rows, aminos, CZ).astype(BF16)
    take(out_all, out_r)
    for view in (near_all, far, side_all, out_all):
        take(view, send_s)


def write_kernel(out_ref, pair_ref, out_hbm, pair_hbm, sem):
    copies = [pltpu.make_async_copy(out_ref, out_hbm, sem.at[0]),
              pltpu.make_async_copy(pair_ref, pair_hbm, sem.at[1])]
    for copy in copies:
        copy.start()
    for copy in copies:
        copy.wait()


def fused(*args):
    emb, mask, resolved, pair = args[:4]
    groups, ranks = lax.axis_size("seq"), lax.axis_size("res")
    chains, aminos = emb.shape[:2]
    per = chains // ranks
    pair_rows = pair.shape[0]
    quads = pair_rows // aminos
    devices = groups * ranks
    folds = 8 // aminos
    operands = (emb.reshape(ranks, per, aminos, ROW_FEATURES), mask.T, resolved.reshape(1, -1), pair, args[4], args[5].T, args[6],
                args[7].T, args[8].reshape(PROJ_FEATURES // folds, folds, PROJ_FEATURES, CZ))
    vmem = pl.BlockSpec(memory_space=pltpu.VMEM)
    whole = pl.BlockSpec(memory_space=pl.ANY)
    dma = pltpu.SemaphoreType.DMA
    results = pl.pallas_call(
        functools.partial(fused_kernel, groups, ranks, per, aminos),
        out_shape=(pltpu.VMEM(emb.shape, BF16), pltpu.VMEM(pair.shape, BF16)),
        in_specs=[whole] * len(operands),
        out_specs=(vmem, vmem),
        scratch_shapes=[
            pltpu.VMEM((ranks, per + 1, aminos, ROW_FEATURES), BF16),
            pltpu.VMEM((per + 1, ranks, aminos, ROW_FEATURES), BF16),
            pltpu.VMEM((ranks, aminos, ROW_FEATURES), BF16),
        ] + [pltpu.VMEM(x.shape, x.dtype) for x in operands[1:8]] + [
            pltpu.VMEM((PROJ_FEATURES // folds, PROJ_FEATURES, folds * CZ), BF16),
            pltpu.VMEM((groups, ranks, quads + 1, per, LANES), BF16),
            pltpu.VMEM((quads + 1, devices, per, LANES), BF16),
            pltpu.VMEM((per, ranks, aminos, ROW_FEATURES), BF16),
            pltpu.VMEM((chains * aminos, ROW_FEATURES), F32),
            pltpu.VMEM((chains * aminos, LANES), F32),
            pltpu.VMEM((chains * aminos, 2 * LANES), F32),
            pltpu.VMEM((chains * aminos, ROW_FEATURES), F32),
            pltpu.VMEM((chains * aminos, ROW_FEATURES), BF16),
            pltpu.VMEM((LANES, per * LANES), BF16),
            pltpu.VMEM((chains, chains * aminos), BF16),
            pltpu.VMEM((2 * LANES, ROW_FEATURES), BF16),
            pltpu.VMEM((pair_rows * aminos, CZ), F32),
            dma((6,)), dma, dma, dma, dma, dma,
        ],
        compiler_params=pltpu.CompilerParams(collective_id=0, has_side_effects=True),
    )(*operands)
    return pl.pallas_call(
        write_kernel,
        out_shape=(jax.ShapeDtypeStruct(emb.shape, BF16), jax.ShapeDtypeStruct(pair.shape, BF16)),
        in_specs=[whole, whole],
        out_specs=(whole, whole),
        scratch_shapes=[dma((2,))],
    )(*[pltpu.with_memory_space_constraint(x, pltpu.VMEM) for x in results])


def fits(mesh, emb, pair):
    groups, ranks = mesh.shape["seq"], mesh.shape["res"]
    chains, aminos = emb.shape[:2]
    if chains % ranks or aminos * PROJ_FEATURES != LANES or chains * aminos != LANES:
        return False
    if ranks & (ranks - 1) or HEAD_NUMBER * PER_HEAD_DIM != groups * LANES:
        return False
    pairs = pair.shape[0] * aminos
    return pairs * groups == LANES and chains // ranks * aminos * groups == PROJ_FEATURES


def solution(mesh):
    placed = (
        P(("crop", "seq"), "res", None),
        P(("crop", "seq"), "res"),
        P("crop"),
        P(("crop", "seq"), "res", None),
        P(),
        P(),
        P(),
        P(),
        P(),
    )
    def either(*args):
        return (fused if fits(mesh, args[0], args[3]) else per_device)(*args)

    return jax.shard_map(
        either,
        mesh=mesh,
        in_specs=placed,
        out_specs=(P(("crop", "seq"), "res", None), P(("crop", "seq"), "res", None)),
        check_vma=False,
    )
```

```python
import functools
import math

import jax
import jax.numpy as jnp
from jax import lax
from jax.experimental import pallas as pl
from jax.experimental.pallas import tpu as pltpu
from jax.sharding import PartitionSpec as P

ROW_FEATURES = 256
CZ = 128
HEAD_NUMBER = 8
PER_HEAD_DIM = 32
PROJ_FEATURES = 32


epsilon = 1e-05


def layer_normalize(values):
    values = values.astype(jnp.float32)
    average = jnp.mean(values, axis=-1, keepdims=True)
    centered = values - average
    variance = jnp.mean(centered * centered, axis=-1, keepdims=True)
    return centered * lax.rsqrt(variance + epsilon)


def outer_rows(left_side, right_side, project):
    row_total = left_side.shape[1]
    col_total = right_side.shape[1]
    block_rows = math.gcd(row_total, max(1, 2048 // col_total))

    def outer_block(start):
        product = jnp.einsum(
            "sic,sje->ijce", left_side, right_side, preferred_element_type=jnp.float32
        )
        flattened = product.reshape(block_rows * col_total, PROJ_FEATURES * PROJ_FEATURES)
        return jnp.dot(flattened, project, precision=lax.Precision.HIGHEST).reshape(
            block_rows, col_total, CZ
        )

    starts = jnp.arange(row_total // block_rows, dtype=jnp.int32) * block_rows
    return lax.map(outer_block, starts).reshape(row_total, col_total, CZ)


def per_device(
    aligned_chain_embedding,
    alignment_mask,
    resolved_residue_mask,
    pairwise_state,
    combined_projection_matrix,
    pair_bias_weight,
    final_projection_matrix,
    left_right_projection_matrix,
    outer_mean_weight,
):
    chain_count = aligned_chain_embedding.shape[0]
    amino_count = aligned_chain_embedding.shape[1]
    res_ranks = lax.axis_size("res")
    seq_groups = lax.axis_size("seq")
    full_length = amino_count * res_ranks
    row_count = full_length // seq_groups
    item_count = HEAD_NUMBER * chain_count // res_ranks
    per_head = min(item_count, chain_count)
    head_count = item_count // per_head
    my_rank = lax.axis_index("res")
    my_group = lax.axis_index("seq")
    standardized_rows = layer_normalize(aligned_chain_embedding).astype(jnp.bfloat16)
    linear_mapped = jnp.dot(
        standardized_rows.reshape(chain_count * amino_count, ROW_FEATURES),
        combined_projection_matrix,
        preferred_element_type=jnp.float32,
    )
    linear_mapped = linear_mapped.reshape(chain_count, amino_count, 4, HEAD_NUMBER, PER_HEAD_DIM)
    queries = (linear_mapped[:, :, 0] * PER_HEAD_DIM ** (-0.5)).astype(jnp.bfloat16)
    key_rows = linear_mapped[:, :, 1].astype(jnp.bfloat16)
    value_rows = linear_mapped[:, :, 2].astype(jnp.bfloat16)
    sigmoid_factor = jax.nn.sigmoid(linear_mapped[:, :, 3])
    stacked = jnp.stack([queries, key_rows, value_rows], axis=2)
    stacked = jnp.transpose(stacked, (3, 0, 1, 2, 4)).reshape(
        HEAD_NUMBER * chain_count, amino_count, 3 * PER_HEAD_DIM
    )
    presence_mask_flags = alignment_mask.astype(jnp.bfloat16)
    key_flags = jnp.broadcast_to(
        presence_mask_flags[None], (HEAD_NUMBER, chain_count, amino_count)
    ).reshape(HEAD_NUMBER * chain_count, amino_count)
    arrived, arrived_flags = (
        lax.all_to_all(stacked, "res", split_axis=0, concat_axis=1, tiled=True),
        lax.all_to_all(key_flags, "res", split_axis=0, concat_axis=1, tiled=True),
    )
    pair_normed = layer_normalize(pairwise_state).astype(jnp.bfloat16)
    local_bias = jnp.dot(
        pair_normed.reshape(row_count * amino_count, CZ),
        pair_bias_weight,
        preferred_element_type=jnp.float32,
    )
    local_bias = jnp.transpose(
        local_bias.astype(jnp.bfloat16).reshape(row_count, amino_count, HEAD_NUMBER), (2, 0, 1)
    )
    bias_cols = lax.all_gather(local_bias, "res", axis=2, tiled=True)
    whole_bias = lax.all_gather(bias_cols, "seq", axis=1, tiled=True)
    first_head = my_rank * item_count // chain_count
    head_bias = lax.dynamic_slice_in_dim(whole_bias, first_head, head_count, 0)
    grouped = arrived.reshape(head_count, per_head, full_length, 3, PER_HEAD_DIM)
    key_validity_mask = (
        arrived_flags.reshape(head_count, per_head, full_length).astype(jnp.float32) - 1.0
    ) * 1000000000.0
    scores = jnp.einsum(
        "gpid,gpjd->gpij",
        grouped[:, :, :, 0],
        grouped[:, :, :, 1],
        preferred_element_type=jnp.float32,
    )
    scores = scores + head_bias.astype(jnp.float32)[:, None] + key_validity_mask[:, :, None, :]
    row_max = jnp.max(scores, axis=-1, keepdims=True)
    exponent = jnp.exp(scores - row_max)
    weights = (exponent / jnp.sum(exponent, axis=-1, keepdims=True)).astype(jnp.bfloat16)
    softmax_mixed = jnp.einsum(
        "gpij,gpjd->gpid", weights, grouped[:, :, :, 2], preferred_element_type=jnp.float32
    )
    softmax_mixed = softmax_mixed.astype(jnp.bfloat16).reshape(
        item_count, full_length, PER_HEAD_DIM
    )
    returned = lax.all_to_all(softmax_mixed, "res", split_axis=1, concat_axis=0, tiled=True)
    returned = jnp.transpose(
        returned.reshape(HEAD_NUMBER, chain_count, amino_count, PER_HEAD_DIM), (1, 2, 0, 3)
    )
    sigmoid_scaled = (
        (sigmoid_factor * returned.astype(jnp.float32))
        .astype(jnp.bfloat16)
        .reshape(chain_count * amino_count, ROW_FEATURES)
    )
    embedding_increment = jnp.dot(
        sigmoid_scaled, final_projection_matrix, preferred_element_type=jnp.float32
    ).reshape(chain_count, amino_count, ROW_FEATURES)
    alignment_output = (aligned_chain_embedding.astype(jnp.float32) + embedding_increment).astype(
        jnp.bfloat16
    )
    standardized_product = layer_normalize(alignment_output).astype(jnp.bfloat16)
    left_right_vectors = jnp.dot(
        standardized_product.reshape(chain_count * amino_count, ROW_FEATURES),
        left_right_projection_matrix,
        preferred_element_type=jnp.float32,
    )
    left_right_vectors = left_right_vectors.reshape(chain_count, amino_count, 2, PROJ_FEATURES)
    entry_present = alignment_mask.astype(jnp.float32)[:, :, None]
    left_side = (left_right_vectors[:, :, 0] * entry_present).astype(jnp.bfloat16)
    right_side = (left_right_vectors[:, :, 1] * entry_present).astype(jnp.bfloat16)
    left_all, left_flags = (
        lax.all_gather(left_side, "res", axis=1, tiled=True),
        lax.all_gather(presence_mask_flags, "res", axis=1, tiled=True),
    )
    project = outer_mean_weight.astype(jnp.float32)
    row_start = my_group * row_count
    left_full, flag_full = (
        lax.all_to_all(left_all, "seq", split_axis=1, concat_axis=0, tiled=True),
        lax.all_to_all(left_flags, "seq", split_axis=1, concat_axis=0, tiled=True),
    )
    right_full, right_flags = (
        lax.all_gather(right_side, "seq", axis=0, tiled=True),
        lax.all_gather(presence_mask_flags, "seq", axis=0, tiled=True),
    )
    counts = jnp.dot(flag_full.T, right_flags, preferred_element_type=jnp.float32)
    outer = outer_rows(left_full, right_full, project)
    col_start = my_rank * amino_count
    row_mask = lax.dynamic_slice_in_dim(resolved_residue_mask, row_start, row_count).astype(
        jnp.float32
    )
    col_mask = lax.dynamic_slice_in_dim(resolved_residue_mask, col_start, amino_count).astype(
        jnp.float32
    )
    pair_mask = row_mask[:, None] * col_mask[None, :]
    pairwise_output = (
        pairwise_state.astype(jnp.float32) + pair_mask[:, :, None] * (outer / counts[:, :, None])
    ).astype(jnp.bfloat16)
    return (alignment_output, pairwise_output)


LANES = 128
F32 = jnp.float32
BF16 = jnp.bfloat16


def iota(shape, axis):
    return lax.broadcasted_iota(jnp.int32, shape, axis)


def dot(a, b, ca=1, cb=0):
    return lax.dot_general(a, b, (((ca,), (cb,)), ((), ())), preferred_element_type=F32)


def one_hot(cond):
    return jnp.where(cond, 1.0, 0.0).astype(BF16)


def flat(block):
    return block.reshape(-1, block.shape[-1])


def turn_blocks(slabs):
    count = len(slabs)
    size = LANES // count
    lane = iota(slabs[0].shape, 1) // size
    slabs = list(slabs)
    half = count // 2
    while half:
        low = lane // half % 2 == 0
        for x in range(count):
            if x // half % 2 == 0:
                a, b = slabs[x], slabs[x + half]
                slabs[x] = jnp.where(low, a, pltpu.roll(b, half * size, 1))
                slabs[x + half] = jnp.where(low, pltpu.roll(a, LANES - half * size, 1), b)
        half //= 2
    return slabs


def fused_kernel(
    groups, ranks, per, aminos,
    emb_hbm, mask_hbm, resolved_hbm, pair_hbm, proj_hbm, bias_hbm, final_hbm, lr_hbm, outer_hbm,
    out_ref, pair_out_ref,
    pack, near, far, mask_ref, resolved_ref, pair_ref, proj_ref, bias_w_ref, final_ref, lr_ref,
    outer_ref, side_send, side_buf, out_send, raw_buf, mask_buf, keep_buf, gate_buf, value_buf,
    pick_ref, gather_ref, sides_w_ref, turn_buf, load_s, send_s, near_r, far_r, flag_r, side_r, out_r,
):
    devices = groups * ranks
    chains = per * ranks
    full = ranks * aminos
    rows = per * full
    pair_rows = full // groups
    pairs = pair_rows * aminos
    quads = pair_rows // aminos
    width = HEAD_NUMBER * PER_HEAD_DIM
    halves = width // LANES
    heads_per = LANES // PER_HEAD_DIM
    slot = LANES // groups
    folds = 8 // aminos
    cores = math.gcd(2, ranks)
    group = lax.axis_index("seq")
    rank = lax.axis_index("res")
    me = group * ranks + rank

    chip, core = rank // cores, rank % cores

    def flip(k):
        peer = 0
        for bit in range((ranks // cores).bit_length() - 1):
            digit = chip // (1 << bit) % 2
            peer = peer + (1 << bit) * (1 - digit if k >> bit & 1 else digit)
        return peer

    others = []
    for shift in range(groups - 1, -1, -1):
        g = lax.rem(group + shift, groups)
        for k in range(ranks // cores - 1, -1, -1):
            for x in range(cores):
                if shift or k:
                    others.append((shift, g, flip(k) * cores + x))
    for x in range(1, cores):
        others.append((0, group, chip * cores + lax.rem(core + x, cores)))

    barrier = pltpu.get_barrier_semaphore()
    for _, g, r in others:
        pl.semaphore_signal(
            barrier, inc=1, device_id={"seq": g, "res": r}, device_id_type=pl.DeviceIdType.MESH
        )

    def load(k, src, dst):
        copy = pltpu.make_async_copy(src, dst, load_s.at[k])
        copy.start()
        return copy

    emb_load = load(0, emb_hbm, pack.at[:, pl.ds(0, per)])
    pair_load = load(1, pair_hbm, pair_ref)
    bias_load = load(2, bias_hbm, bias_w_ref)
    mask_load = load(3, mask_hbm, mask_ref)
    proj_load = load(4, proj_hbm, proj_ref)
    final_load = load(4, final_hbm, final_ref)
    lr_load = load(4, lr_hbm, lr_ref)
    resolved_load = load(4, resolved_hbm, resolved_ref)
    for x in range(folds):
        load(5, outer_hbm.at[:, x], outer_ref.at[:, :, pl.ds(x * CZ, CZ)])

    def send(src, dst, rsem, g, r):
        pltpu.make_async_remote_copy(
            src_ref=src, dst_ref=dst, send_sem=send_s, recv_sem=rsem,
            device_id={"seq": g, "res": r}, device_id_type=pl.DeviceIdType.MESH,
        ).start()

    def take(view, sem):
        pltpu.make_async_copy(view, view, sem).wait()

    own = pl.ds(rank * per, per)
    low, high = pl.ds(0, LANES), pl.ds(LANES, LANES)
    near_all = near.at[:, pl.ds(0, ranks - 1)]
    side_all = side_buf.at[:, pl.ds(0, devices - 1)]
    out_all = out_ref.at[pl.ds(0, per * (ranks - 1))]

    bias_load.wait()
    lane_head = iota((LANES, HEAD_NUMBER), 0)
    lane_head = (lane_head // slot + group) % groups * heads_per + lane_head % slot // pair_rows
    wide_w = dot(one_hot(lane_head == iota((LANES, HEAD_NUMBER), 1)), bias_w_ref[...]).astype(BF16)
    mask_load.wait()
    flags = dot(mask_ref[...].astype(F32).astype(BF16), one_hot(
        iota((chains, LANES), 0) == iota((chains, LANES), 1)))
    pair_load.wait()
    pair_value = flat(pair_ref[...].astype(F32))
    own_bias = dot(layer_normalize(pair_value).astype(BF16), wide_w, 1, 1)
    own_bias = jnp.where(
        iota((pairs, LANES), 0) // aminos == iota((pairs, LANES), 1) % pair_rows, own_bias, 0.0)
    own_bias = jnp.sum(own_bias.reshape(pair_rows, aminos, LANES), axis=0)
    aux = jnp.concatenate([own_bias, flags], axis=1).astype(BF16)
    for r in range(ranks):
        pack[r, per] = aux
    emb_load.wait()
    near[:, pl.ds(rank, 1)] = pack[rank][:, None]

    pl.semaphore_wait(barrier, devices - 1)
    for shift, g, r in others:
        if shift:
            send(pack.at[0, per, :, low], far.at[rank, :, low], far_r, g, r)
        else:
            send(pack.at[r], near.at[:, rank], near_r, g, r)
    for copy in (proj_load, final_load, lr_load, resolved_load):
        copy.wait()
    block_mask = (iota((LANES, LANES), 0) % slot // pair_rows
                  == iota((LANES, LANES), 1) // PER_HEAD_DIM)
    at = (LANES, per * LANES)
    pick_ref[...] = one_hot(iota(at, 0) == rank * per + iota(at, 1) // LANES)
    at = (chains, rows)
    gather_ref[...] = one_hot((iota(at, 0) // per == iota(at, 1) % full // aminos)
                              & (iota(at, 0) % per == iota(at, 1) // full))
    at = (2 * LANES, 2 * PROJ_FEATURES)
    left_row, right_row = iota(at, 0) // aminos, PROJ_FEATURES + iota(at, 0) % PROJ_FEATURES
    sides_w_ref[...] = dot(one_hot(
        jnp.where(iota(at, 0) < LANES, left_row, right_row) == iota(at, 1)), lr_ref[...]).astype(BF16)
    two = (rows, 2 * LANES)
    amino = jnp.where(iota(two, 1) < LANES, iota(two, 1) % aminos,
                      iota(two, 1) % LANES // PROJ_FEATURES)
    keep_buf[...] = jnp.where(amino == iota(two, 0) % aminos, 1.0, 0.0)
    for shift, g, r in others:
        if shift:
            send(pack.at[0, per, :, high], far.at[rank, :, high], flag_r, g, r)
    take(near_all, near_r)
    embedding = near[:per].astype(F32).reshape(rows, ROW_FEATURES)
    normed = layer_normalize(embedding).astype(BF16)
    projected = dot(normed, proj_ref[...])
    queries = (projected[:, :width] * PER_HEAD_DIM ** (-0.5)).astype(BF16)
    keys = projected[:, width:2 * width].astype(BF16)
    value_buf[...] = projected[:, 2 * width:3 * width].astype(BF16)
    gate_buf[...] = jax.nn.sigmoid(projected[:, 3 * width:])

    for b in range(halves):
        cols = slice(b * LANES, (b + 1) * LANES)
        for c in range(per):
            spread = []
            for s in range(groups):
                at = c * full + (b - s) % groups * pair_rows
                spread += [queries[at:at + pair_rows, cols]] * heads_per
            spread = jnp.concatenate(spread, axis=0)
            spread = jnp.where(block_mask, spread, jnp.zeros_like(spread))
            raw_buf[c * full:(c + 1) * full, cols] = dot(
                keys[c * full:(c + 1) * full, cols], spread, 1, 1)

    near_aux = flat(near[per])
    key_flags = dot(near_aux[:, LANES:], pick_ref[...])
    for c in range(per):
        at = slice(c * full, (c + 1) * full)
        present = key_flags[:, c * LANES:(c + 1) * LANES]
        mask_buf[at, :] = (present - 1.0) * 1000000000.0
        keep_buf[at, :] = keep_buf[at, :] * jnp.concatenate([present] * 2, axis=1)
    take(far.at[:, :, low], far_r)
    far_bias = flat(far[:, :, :LANES]).astype(F32)
    near_bias = near_aux[:, :LANES].astype(F32)
    which = iota((full, LANES), 1) // slot
    mixed = []
    for b in range(halves):
        cols = slice(b * LANES, (b + 1) * LANES)
        tile_bias = jnp.where((b + which) % groups == group, near_bias, far_bias)
        weights, blocks = [], []
        for c in range(per):
            at = slice(c * full, (c + 1) * full)
            scores = raw_buf[at, cols] + tile_bias + mask_buf[at, :]
            exponent = jnp.exp(scores - jnp.max(scores, axis=0, keepdims=True))
            total = 1.0 / jnp.sum(exponent, axis=0, keepdims=True)
            weights.append((exponent * total).astype(BF16))
            own_values = value_buf[at, cols]
            blocks.append(jnp.concatenate(
                [own_values if d == c else jnp.zeros_like(own_values) for d in range(per)], axis=1))
        weights = jnp.concatenate(weights, axis=0)
        blocks = jnp.concatenate(blocks, axis=0)
        summed = dot(weights, blocks, 0, 0)
        lane_h = iota((pair_rows, LANES), 1) // PER_HEAD_DIM
        parts = []
        for c in range(per):
            for g in range(groups):
                at = (b - g) % groups * slot
                part = summed[at:at + pair_rows, c * LANES:(c + 1) * LANES]
                for h in range(1, heads_per):
                    row = at + h * pair_rows
                    part = jnp.where(
                        lane_h == h,
                        summed[row:row + pair_rows, c * LANES:(c + 1) * LANES], part)
                parts.append(part)
        mixed.append(jnp.concatenate(parts, axis=0))
    attended = jnp.concatenate(mixed, axis=1).astype(BF16)
    gated = (gate_buf[...] * attended.astype(F32)).astype(BF16)
    updated = (embedding + dot(gated, final_ref[...])).astype(BF16)
    out_send[...] = updated.astype(F32).reshape(per, ranks, aminos, ROW_FEATURES).astype(BF16)
    normed_out = layer_normalize(updated).astype(BF16)
    sides = (dot(normed_out, sides_w_ref[...], 1, 1) * keep_buf[...]).astype(BF16)
    sides = dot(gather_ref[...], sides).reshape(ranks, per, 2 * LANES).astype(BF16)
    left = sides[:, :, :LANES].reshape(groups, quads, per, LANES)
    right = sides[:, :, LANES:]
    def fill(start, stop):
        for r in range(start, stop):
            side_send[:, r, :quads] = left
        for g in range(groups):
            side_send[g, start:stop, quads] = right[start:stop]

    fill(0, 2 * cores)
    place = rank // cores * groups * cores + group * cores + lax.rem(rank, cores)
    for n in range(devices - 1):
        at = n + lax.div(n - place + devices, devices)
        g = lax.rem(lax.div(at, cores), groups)
        r = lax.div(at, groups * cores) * cores + lax.rem(at, cores)
        send(side_send.at[g, r], side_buf.at[:, me], side_r, g, r)
        if n == cores - 1:
            fill(2 * cores, ranks)
        if n % (groups * cores) == cores - 1:
            for m in range(n // groups // cores * cores, n // groups // cores * cores + cores):
                if m < ranks - 1:
                    r = m + lax.div(m - rank + ranks, ranks)
                    send(out_send.at[:, r], out_ref.at[own], out_r, group, r)
    side_buf[:, pl.ds(me, 1)] = side_send[group, rank][:, None]
    out_ref[own] = out_send[:, pl.ds(rank, 1)].reshape(per, aminos, ROW_FEATURES)

    at = (pairs, full)
    row_pick = iota(at, 1) == group * pair_rows + iota(at, 0) // aminos
    col_pick = iota(at, 1) == rank * aminos + iota(at, 0) % aminos
    both = jnp.zeros((pairs, LANES), F32)
    take(far.at[:, :, high], flag_r)
    for seen in (near_aux[:, LANES:], flat(far[:, :, LANES:])):
        both = both + dot(one_hot(row_pick), seen) * dot(one_hot(col_pick), seen)
    counts = jnp.sum(both, axis=1, keepdims=True)
    resolved = jnp.broadcast_to(resolved_ref[...].astype(F32), at)
    scale = jnp.sum(jnp.where(row_pick, resolved, 0.0), axis=1, keepdims=True) * jnp.sum(
        jnp.where(col_pick, resolved, 0.0), axis=1, keepdims=True) / counts
    scale = jnp.broadcast_to(scale, (pairs, LANES))
    take(outer_ref, load_s.at[5])
    take(side_all, side_r)
    right_rows = flat(side_buf[quads])
    products = [dot(flat(side_buf[q]), right_rows, 0, 0) for q in range(quads)]
    parts = []
    step = folds * aminos
    for c in range(0, PROJ_FEATURES // folds, aminos):
        slabs = []
        for x in range(c, c + aminos):
            slab = [product[x * step:(x + 1) * step] for product in products]
            slabs.append(jnp.concatenate(slab, axis=0).astype(BF16))
        parts.append(jnp.concatenate(turn_blocks(slabs), axis=0))
    outer = dot(jnp.concatenate(parts, axis=1), outer_ref[...].reshape(-1, folds * CZ))
    for j in range(aminos):
        for q in range(quads):
            base = (j * quads + q) * folds * aminos
            total = outer[base:base + aminos, :CZ]
            for x in range(1, folds):
                row = base + x * aminos
                total = total + outer[row:row + aminos, x * CZ:(x + 1) * CZ]
            turn_buf[pl.ds(q * aminos * aminos + j, aminos, stride=aminos), :] = total
    result = pair_value + scale * turn_buf[...]
    pair_out_ref[...] = result.reshape(pair_rows, aminos, CZ).astype(BF16)
    take(out_all, out_r)
    for view in (near_all, far, side_all, out_all):
        take(view, send_s)


def write_kernel(out_ref, pair_ref, out_hbm, pair_hbm, sem):
    copies = [pltpu.make_async_copy(out_ref, out_hbm, sem.at[0]),
              pltpu.make_async_copy(pair_ref, pair_hbm, sem.at[1])]
    for copy in copies:
        copy.start()
    for copy in copies:
        copy.wait()


def fused(*args):
    emb, mask, resolved, pair = args[:4]
    groups, ranks = lax.axis_size("seq"), lax.axis_size("res")
    chains, aminos = emb.shape[:2]
    per = chains // ranks
    pair_rows = pair.shape[0]
    quads = pair_rows // aminos
    devices = groups * ranks
    folds = 8 // aminos
    operands = (emb.reshape(ranks, per, aminos, ROW_FEATURES), mask.T, resolved.reshape(1, -1), pair, args[4], args[5].T, args[6],
                args[7].T, args[8].reshape(PROJ_FEATURES // folds, folds, PROJ_FEATURES, CZ))
    vmem = pl.BlockSpec(memory_space=pltpu.VMEM)
    whole = pl.BlockSpec(memory_space=pl.ANY)
    dma = pltpu.SemaphoreType.DMA
    results = pl.pallas_call(
        functools.partial(fused_kernel, groups, ranks, per, aminos),
        out_shape=(pltpu.VMEM(emb.shape, BF16), pltpu.VMEM(pair.shape, BF16)),
        in_specs=[whole] * len(operands),
        out_specs=(vmem, vmem),
        scratch_shapes=[
            pltpu.VMEM((ranks, per + 1, aminos, ROW_FEATURES), BF16),
            pltpu.VMEM((per + 1, ranks, aminos, ROW_FEATURES), BF16),
            pltpu.VMEM((ranks, aminos, ROW_FEATURES), BF16),
        ] + [pltpu.VMEM(x.shape, x.dtype) for x in operands[1:8]] + [
            pltpu.VMEM((PROJ_FEATURES // folds, PROJ_FEATURES, folds * CZ), BF16),
            pltpu.VMEM((groups, ranks, quads + 1, per, LANES), BF16),
            pltpu.VMEM((quads + 1, devices, per, LANES), BF16),
            pltpu.VMEM((per, ranks, aminos, ROW_FEATURES), BF16),
            pltpu.VMEM((chains * aminos, ROW_FEATURES), F32),
            pltpu.VMEM((chains * aminos, LANES), F32),
            pltpu.VMEM((chains * aminos, 2 * LANES), F32),
            pltpu.VMEM((chains * aminos, ROW_FEATURES), F32),
            pltpu.VMEM((chains * aminos, ROW_FEATURES), BF16),
            pltpu.VMEM((LANES, per * LANES), BF16),
            pltpu.VMEM((chains, chains * aminos), BF16),
            pltpu.VMEM((2 * LANES, ROW_FEATURES), BF16),
            pltpu.VMEM((pair_rows * aminos, CZ), F32),
            dma((6,)), dma, dma, dma, dma, dma, dma,
        ],
        compiler_params=pltpu.CompilerParams(collective_id=0, has_side_effects=True),
    )(*operands)
    return pl.pallas_call(
        write_kernel,
        out_shape=(jax.ShapeDtypeStruct(emb.shape, BF16), jax.ShapeDtypeStruct(pair.shape, BF16)),
        in_specs=[whole, whole],
        out_specs=(whole, whole),
        scratch_shapes=[dma((2,))],
    )(*[pltpu.with_memory_space_constraint(x, pltpu.VMEM) for x in results])


def fits(mesh, emb, pair):
    groups, ranks = mesh.shape["seq"], mesh.shape["res"]
    chains, aminos = emb.shape[:2]
    if chains % ranks or aminos * PROJ_FEATURES != LANES or chains * aminos != LANES:
        return False
    if ranks & (ranks - 1) or HEAD_NUMBER * PER_HEAD_DIM != groups * LANES:
        return False
    pairs = pair.shape[0] * aminos
    return pairs * groups == LANES and chains // ranks * aminos * groups == PROJ_FEATURES


def solution(mesh):
    placed = (
        P(("crop", "seq"), "res", None),
        P(("crop", "seq"), "res"),
        P("crop"),
        P(("crop", "seq"), "res", None),
        P(),
        P(),
        P(),
        P(),
        P(),
    )
    def either(*args):
        return (fused if fits(mesh, args[0], args[3]) else per_device)(*args)

    return jax.shard_map(
        either,
        mesh=mesh,
        in_specs=placed,
        out_specs=(P(("crop", "seq"), "res", None), P(("crop", "seq"), "res", None)),
        check_vma=False,
    )
```

```python
import functools
import math

import jax
import jax.numpy as jnp
from jax import lax
from jax.experimental import pallas as pl
from jax.experimental.pallas import tpu as pltpu
from jax.sharding import PartitionSpec as P

ROW_FEATURES = 256
CZ = 128
HEAD_NUMBER = 8
PER_HEAD_DIM = 32
PROJ_FEATURES = 32


epsilon = 1e-05


def layer_normalize(values):
    values = values.astype(jnp.float32)
    average = jnp.mean(values, axis=-1, keepdims=True)
    centered = values - average
    variance = jnp.mean(centered * centered, axis=-1, keepdims=True)
    return centered * lax.rsqrt(variance + epsilon)


def outer_rows(left_side, right_side, project):
    row_total = left_side.shape[1]
    col_total = right_side.shape[1]
    block_rows = math.gcd(row_total, max(1, 2048 // col_total))

    def outer_block(start):
        product = jnp.einsum(
            "sic,sje->ijce", left_side, right_side, preferred_element_type=jnp.float32
        )
        flattened = product.reshape(block_rows * col_total, PROJ_FEATURES * PROJ_FEATURES)
        return jnp.dot(flattened, project, precision=lax.Precision.HIGHEST).reshape(
            block_rows, col_total, CZ
        )

    starts = jnp.arange(row_total // block_rows, dtype=jnp.int32) * block_rows
    return lax.map(outer_block, starts).reshape(row_total, col_total, CZ)


def per_device(
    aligned_chain_embedding,
    alignment_mask,
    resolved_residue_mask,
    pairwise_state,
    combined_projection_matrix,
    pair_bias_weight,
    final_projection_matrix,
    left_right_projection_matrix,
    outer_mean_weight,
):
    chain_count = aligned_chain_embedding.shape[0]
    amino_count = aligned_chain_embedding.shape[1]
    res_ranks = lax.axis_size("res")
    seq_groups = lax.axis_size("seq")
    full_length = amino_count * res_ranks
    row_count = full_length // seq_groups
    item_count = HEAD_NUMBER * chain_count // res_ranks
    per_head = min(item_count, chain_count)
    head_count = item_count // per_head
    my_rank = lax.axis_index("res")
    my_group = lax.axis_index("seq")
    standardized_rows = layer_normalize(aligned_chain_embedding).astype(jnp.bfloat16)
    linear_mapped = jnp.dot(
        standardized_rows.reshape(chain_count * amino_count, ROW_FEATURES),
        combined_projection_matrix,
        preferred_element_type=jnp.float32,
    )
    linear_mapped = linear_mapped.reshape(chain_count, amino_count, 4, HEAD_NUMBER, PER_HEAD_DIM)
    queries = (linear_mapped[:, :, 0] * PER_HEAD_DIM ** (-0.5)).astype(jnp.bfloat16)
    key_rows = linear_mapped[:, :, 1].astype(jnp.bfloat16)
    value_rows = linear_mapped[:, :, 2].astype(jnp.bfloat16)
    sigmoid_factor = jax.nn.sigmoid(linear_mapped[:, :, 3])
    stacked = jnp.stack([queries, key_rows, value_rows], axis=2)
    stacked = jnp.transpose(stacked, (3, 0, 1, 2, 4)).reshape(
        HEAD_NUMBER * chain_count, amino_count, 3 * PER_HEAD_DIM
    )
    presence_mask_flags = alignment_mask.astype(jnp.bfloat16)
    key_flags = jnp.broadcast_to(
        presence_mask_flags[None], (HEAD_NUMBER, chain_count, amino_count)
    ).reshape(HEAD_NUMBER * chain_count, amino_count)
    arrived, arrived_flags = (
        lax.all_to_all(stacked, "res", split_axis=0, concat_axis=1, tiled=True),
        lax.all_to_all(key_flags, "res", split_axis=0, concat_axis=1, tiled=True),
    )
    pair_normed = layer_normalize(pairwise_state).astype(jnp.bfloat16)
    local_bias = jnp.dot(
        pair_normed.reshape(row_count * amino_count, CZ),
        pair_bias_weight,
        preferred_element_type=jnp.float32,
    )
    local_bias = jnp.transpose(
        local_bias.astype(jnp.bfloat16).reshape(row_count, amino_count, HEAD_NUMBER), (2, 0, 1)
    )
    bias_cols = lax.all_gather(local_bias, "res", axis=2, tiled=True)
    whole_bias = lax.all_gather(bias_cols, "seq", axis=1, tiled=True)
    first_head = my_rank * item_count // chain_count
    head_bias = lax.dynamic_slice_in_dim(whole_bias, first_head, head_count, 0)
    grouped = arrived.reshape(head_count, per_head, full_length, 3, PER_HEAD_DIM)
    key_validity_mask = (
        arrived_flags.reshape(head_count, per_head, full_length).astype(jnp.float32) - 1.0
    ) * 1000000000.0
    scores = jnp.einsum(
        "gpid,gpjd->gpij",
        grouped[:, :, :, 0],
        grouped[:, :, :, 1],
        preferred_element_type=jnp.float32,
    )
    scores = scores + head_bias.astype(jnp.float32)[:, None] + key_validity_mask[:, :, None, :]
    row_max = jnp.max(scores, axis=-1, keepdims=True)
    exponent = jnp.exp(scores - row_max)
    weights = (exponent / jnp.sum(exponent, axis=-1, keepdims=True)).astype(jnp.bfloat16)
    softmax_mixed = jnp.einsum(
        "gpij,gpjd->gpid", weights, grouped[:, :, :, 2], preferred_element_type=jnp.float32
    )
    softmax_mixed = softmax_mixed.astype(jnp.bfloat16).reshape(
        item_count, full_length, PER_HEAD_DIM
    )
    returned = lax.all_to_all(softmax_mixed, "res", split_axis=1, concat_axis=0, tiled=True)
    returned = jnp.transpose(
        returned.reshape(HEAD_NUMBER, chain_count, amino_count, PER_HEAD_DIM), (1, 2, 0, 3)
    )
    sigmoid_scaled = (
        (sigmoid_factor * returned.astype(jnp.float32))
        .astype(jnp.bfloat16)
        .reshape(chain_count * amino_count, ROW_FEATURES)
    )
    embedding_increment = jnp.dot(
        sigmoid_scaled, final_projection_matrix, preferred_element_type=jnp.float32
    ).reshape(chain_count, amino_count, ROW_FEATURES)
    alignment_output = (aligned_chain_embedding.astype(jnp.float32) + embedding_increment).astype(
        jnp.bfloat16
    )
    standardized_product = layer_normalize(alignment_output).astype(jnp.bfloat16)
    left_right_vectors = jnp.dot(
        standardized_product.reshape(chain_count * amino_count, ROW_FEATURES),
        left_right_projection_matrix,
        preferred_element_type=jnp.float32,
    )
    left_right_vectors = left_right_vectors.reshape(chain_count, amino_count, 2, PROJ_FEATURES)
    entry_present = alignment_mask.astype(jnp.float32)[:, :, None]
    left_side = (left_right_vectors[:, :, 0] * entry_present).astype(jnp.bfloat16)
    right_side = (left_right_vectors[:, :, 1] * entry_present).astype(jnp.bfloat16)
    left_all, left_flags = (
        lax.all_gather(left_side, "res", axis=1, tiled=True),
        lax.all_gather(presence_mask_flags, "res", axis=1, tiled=True),
    )
    project = outer_mean_weight.astype(jnp.float32)
    row_start = my_group * row_count
    left_full, flag_full = (
        lax.all_to_all(left_all, "seq", split_axis=1, concat_axis=0, tiled=True),
        lax.all_to_all(left_flags, "seq", split_axis=1, concat_axis=0, tiled=True),
    )
    right_full, right_flags = (
        lax.all_gather(right_side, "seq", axis=0, tiled=True),
        lax.all_gather(presence_mask_flags, "seq", axis=0, tiled=True),
    )
    counts = jnp.dot(flag_full.T, right_flags, preferred_element_type=jnp.float32)
    outer = outer_rows(left_full, right_full, project)
    col_start = my_rank * amino_count
    row_mask = lax.dynamic_slice_in_dim(resolved_residue_mask, row_start, row_count).astype(
        jnp.float32
    )
    col_mask = lax.dynamic_slice_in_dim(resolved_residue_mask, col_start, amino_count).astype(
        jnp.float32
    )
    pair_mask = row_mask[:, None] * col_mask[None, :]
    pairwise_output = (
        pairwise_state.astype(jnp.float32) + pair_mask[:, :, None] * (outer / counts[:, :, None])
    ).astype(jnp.bfloat16)
    return (alignment_output, pairwise_output)


LANES = 128
F32 = jnp.float32
BF16 = jnp.bfloat16


def iota(shape, axis):
    return lax.broadcasted_iota(jnp.int32, shape, axis)


def dot(a, b, ca=1, cb=0):
    return lax.dot_general(a, b, (((ca,), (cb,)), ((), ())), preferred_element_type=F32)


def one_hot(cond):
    return jnp.where(cond, 1.0, 0.0).astype(BF16)


def flat(block):
    return block.reshape(-1, block.shape[-1])


def turn_blocks(slabs):
    count = len(slabs)
    size = LANES // count
    lane = iota(slabs[0].shape, 1) // size
    slabs = list(slabs)
    half = count // 2
    while half:
        low = lane // half % 2 == 0
        for x in range(count):
            if x // half % 2 == 0:
                a, b = slabs[x], slabs[x + half]
                slabs[x] = jnp.where(low, a, pltpu.roll(b, half * size, 1))
                slabs[x + half] = jnp.where(low, pltpu.roll(a, LANES - half * size, 1), b)
        half //= 2
    return slabs


def fused_kernel(
    groups, ranks, per, aminos,
    emb_hbm, mask_hbm, resolved_hbm, pair_hbm, proj_hbm, bias_hbm, final_hbm, lr_hbm, outer_hbm,
    out_ref, pair_out_ref,
    pack, near, far, mask_ref, resolved_ref, pair_ref, proj_ref, bias_w_ref, final_ref, lr_ref,
    outer_ref, side_send, side_buf, out_send, raw_buf, mask_buf, keep_buf, gate_buf, value_buf,
    pick_ref, gather_ref, sides_w_ref, turn_buf, load_s, send_s, near_r, far_r, flag_r, side_r, out_r,
):
    devices = groups * ranks
    chains = per * ranks
    full = ranks * aminos
    rows = per * full
    pair_rows = full // groups
    pairs = pair_rows * aminos
    quads = pair_rows // aminos
    width = HEAD_NUMBER * PER_HEAD_DIM
    halves = width // LANES
    heads_per = LANES // PER_HEAD_DIM
    slot = LANES // groups
    folds = 8 // aminos
    cores = math.gcd(2, ranks)
    group = lax.axis_index("seq")
    rank = lax.axis_index("res")
    me = group * ranks + rank

    chip, core = rank // cores, rank % cores

    def flip(k):
        peer = 0
        for bit in range((ranks // cores).bit_length() - 1):
            digit = chip // (1 << bit) % 2
            peer = peer + (1 << bit) * (1 - digit if k >> bit & 1 else digit)
        return peer

    others = []
    for shift in range(groups - 1, -1, -1):
        g = lax.rem(group + shift, groups)
        for k in range(ranks // cores - 1, -1, -1):
            for x in range(cores):
                if shift or k:
                    others.append((shift, g, flip(k) * cores + x))
    for x in range(1, cores):
        others.append((0, group, chip * cores + lax.rem(core + x, cores)))

    barrier = pltpu.get_barrier_semaphore()
    ahead = (groups - 1) * ranks
    for _, g, r in others[:cores] + others[ahead:ahead + cores] + others[cores:ahead] + others[ahead + cores:]:
        pl.semaphore_signal(
            barrier, inc=1, device_id={"seq": g, "res": r}, device_id_type=pl.DeviceIdType.MESH
        )

    def load(k, src, dst):
        copy = pltpu.make_async_copy(src, dst, load_s.at[k])
        copy.start()
        return copy

    emb_load = load(0, emb_hbm, pack.at[:, pl.ds(0, per)])
    pair_load = load(1, pair_hbm, pair_ref)
    bias_load = load(2, bias_hbm, bias_w_ref)
    mask_load = load(3, mask_hbm, mask_ref)
    proj_load = load(4, proj_hbm, proj_ref)
    final_load = load(4, final_hbm, final_ref)
    lr_load = load(4, lr_hbm, lr_ref)
    resolved_load = load(4, resolved_hbm, resolved_ref)
    for x in range(folds):
        load(5, outer_hbm.at[:, x], outer_ref.at[:, :, pl.ds(x * CZ, CZ)])

    def send(src, dst, rsem, g, r):
        pltpu.make_async_remote_copy(
            src_ref=src, dst_ref=dst, send_sem=send_s, recv_sem=rsem,
            device_id={"seq": g, "res": r}, device_id_type=pl.DeviceIdType.MESH,
        ).start()

    def take(view, sem):
        pltpu.make_async_copy(view, view, sem).wait()

    own = pl.ds(rank * per, per)
    low, high = pl.ds(0, LANES), pl.ds(LANES, LANES)
    near_all = near.at[:, pl.ds(0, ranks - 1)]
    side_all = side_buf.at[:, pl.ds(0, devices - 1)]
    out_all = out_ref.at[pl.ds(0, per * (ranks - 1))]

    bias_load.wait()
    lane_head = iota((LANES, HEAD_NUMBER), 0)
    lane_head = (lane_head // slot + group) % groups * heads_per + lane_head % slot // pair_rows
    wide_w = dot(one_hot(lane_head == iota((LANES, HEAD_NUMBER), 1)), bias_w_ref[...]).astype(BF16)
    mask_load.wait()
    flags = dot(mask_ref[...].astype(F32).astype(BF16), one_hot(
        iota((chains, LANES), 0) == iota((chains, LANES), 1)))
    pair_load.wait()
    pair_value = flat(pair_ref[...].astype(F32))
    own_bias = dot(layer_normalize(pair_value).astype(BF16), wide_w, 1, 1)
    own_bias = jnp.where(
        iota((pairs, LANES), 0) // aminos == iota((pairs, LANES), 1) % pair_rows, own_bias, 0.0)
    own_bias = jnp.sum(own_bias.reshape(pair_rows, aminos, LANES), axis=0)
    aux = jnp.concatenate([own_bias, flags], axis=1).astype(BF16)
    for r in range(ranks):
        pack[r, per] = aux
    emb_load.wait()
    near[:, pl.ds(rank, 1)] = pack[rank][:, None]

    pl.semaphore_wait(barrier, devices - 1)
    for shift, g, r in others:
        if shift:
            send(pack.at[0, per, :, low], far.at[rank, :, low], far_r, g, r)
        else:
            send(pack.at[r], near.at[:, rank], near_r, g, r)
    for copy in (proj_load, final_load, lr_load, resolved_load):
        copy.wait()
    block_mask = (iota((LANES, LANES), 0) % slot // pair_rows
                  == iota((LANES, LANES), 1) // PER_HEAD_DIM)
    at = (LANES, per * LANES)
    pick_ref[...] = one_hot(iota(at, 0) == rank * per + iota(at, 1) // LANES)
    at = (chains, rows)
    gather_ref[...] = one_hot((iota(at, 0) // per == iota(at, 1) % full // aminos)
                              & (iota(at, 0) % per == iota(at, 1) // full))
    at = (2 * LANES, 2 * PROJ_FEATURES)
    left_row, right_row = iota(at, 0) // aminos, PROJ_FEATURES + iota(at, 0) % PROJ_FEATURES
    sides_w_ref[...] = dot(one_hot(
        jnp.where(iota(at, 0) < LANES, left_row, right_row) == iota(at, 1)), lr_ref[...]).astype(BF16)
    two = (rows, 2 * LANES)
    amino = jnp.where(iota(two, 1) < LANES, iota(two, 1) % aminos,
                      iota(two, 1) % LANES // PROJ_FEATURES)
    keep_buf[...] = jnp.where(amino == iota(two, 0) % aminos, 1.0, 0.0)
    for shift, g, r in others:
        if shift:
            send(pack.at[0, per, :, high], far.at[rank, :, high], flag_r, g, r)
    take(near_all, near_r)
    embedding = near[:per].astype(F32).reshape(rows, ROW_FEATURES)
    normed = layer_normalize(embedding).astype(BF16)
    projected = dot(normed, proj_ref[...])
    queries = (projected[:, :width] * PER_HEAD_DIM ** (-0.5)).astype(BF16)
    keys = projected[:, width:2 * width].astype(BF16)
    value_buf[...] = projected[:, 2 * width:3 * width].astype(BF16)
    gate_buf[...] = jax.nn.sigmoid(projected[:, 3 * width:])

    for b in range(halves):
        cols = slice(b * LANES, (b + 1) * LANES)
        for c in range(per):
            spread = []
            for s in range(groups):
                at = c * full + (b - s) % groups * pair_rows
                spread += [queries[at:at + pair_rows, cols]] * heads_per
            spread = jnp.concatenate(spread, axis=0)
            spread = jnp.where(block_mask, spread, jnp.zeros_like(spread))
            raw_buf[c * full:(c + 1) * full, cols] = dot(
                keys[c * full:(c + 1) * full, cols], spread, 1, 1)

    near_aux = flat(near[per])
    key_flags = dot(near_aux[:, LANES:], pick_ref[...])
    for c in range(per):
        at = slice(c * full, (c + 1) * full)
        present = key_flags[:, c * LANES:(c + 1) * LANES]
        mask_buf[at, :] = (present - 1.0) * 1000000000.0
        keep_buf[at, :] = keep_buf[at, :] * jnp.concatenate([present] * 2, axis=1)
    take(far.at[:, :, low], far_r)
    far_bias = flat(far[:, :, :LANES]).astype(F32)
    near_bias = near_aux[:, :LANES].astype(F32)
    which = iota((full, LANES), 1) // slot
    mixed = []
    for b in range(halves):
        cols = slice(b * LANES, (b + 1) * LANES)
        tile_bias = jnp.where((b + which) % groups == group, near_bias, far_bias)
        weights, blocks = [], []
        for c in range(per):
            at = slice(c * full, (c + 1) * full)
            scores = raw_buf[at, cols] + tile_bias + mask_buf[at, :]
            exponent = jnp.exp(scores - jnp.max(scores, axis=0, keepdims=True))
            total = 1.0 / jnp.sum(exponent, axis=0, keepdims=True)
            weights.append((exponent * total).astype(BF16))
            own_values = value_buf[at, cols]
            blocks.append(jnp.concatenate(
                [own_values if d == c else jnp.zeros_like(own_values) for d in range(per)], axis=1))
        weights = jnp.concatenate(weights, axis=0)
        blocks = jnp.concatenate(blocks, axis=0)
        summed = dot(weights, blocks, 0, 0)
        lane_h = iota((pair_rows, LANES), 1) // PER_HEAD_DIM
        parts = []
        for c in range(per):
            for g in range(groups):
                at = (b - g) % groups * slot
                part = summed[at:at + pair_rows, c * LANES:(c + 1) * LANES]
                for h in range(1, heads_per):
                    row = at + h * pair_rows
                    part = jnp.where(
                        lane_h == h,
                        summed[row:row + pair_rows, c * LANES:(c + 1) * LANES], part)
                parts.append(part)
        mixed.append(jnp.concatenate(parts, axis=0))
    attended = jnp.concatenate(mixed, axis=1).astype(BF16)
    gated = (gate_buf[...] * attended.astype(F32)).astype(BF16)
    updated = (embedding + dot(gated, final_ref[...])).astype(BF16)
    out_send[...] = updated.astype(F32).reshape(per, ranks, aminos, ROW_FEATURES).astype(BF16)
    normed_out = layer_normalize(updated).astype(BF16)
    sides = (dot(normed_out, sides_w_ref[...], 1, 1) * keep_buf[...]).astype(BF16)
    sides = dot(gather_ref[...], sides).reshape(ranks, per, 2 * LANES).astype(BF16)
    left = sides[:, :, :LANES].reshape(groups, quads, per, LANES)
    right = sides[:, :, LANES:]
    def fill(start, stop):
        for r in range(start, stop):
            side_send[:, r, :quads] = left
        for g in range(groups):
            side_send[g, start:stop, quads] = right[start:stop]

    fill(0, 2 * cores)
    place = rank // cores * groups * cores + group * cores + lax.rem(rank, cores)
    for n in range(devices - 1):
        at = n + lax.div(n - place + devices, devices)
        g = lax.rem(lax.div(at, cores), groups)
        r = lax.div(at, groups * cores) * cores + lax.rem(at, cores)
        send(side_send.at[g, r], side_buf.at[:, me], side_r, g, r)
        if n == cores - 1:
            fill(2 * cores, ranks)
        if n % (groups * cores) == cores - 1:
            for m in range(n // groups // cores * cores, n // groups // cores * cores + cores):
                if m < ranks - 1:
                    r = m + lax.div(m - rank + ranks, ranks)
                    send(out_send.at[:, r], out_ref.at[own], out_r, group, r)
    side_buf[:, pl.ds(me, 1)] = side_send[group, rank][:, None]
    out_ref[own] = out_send[:, pl.ds(rank, 1)].reshape(per, aminos, ROW_FEATURES)

    at = (pairs, full)
    row_pick = iota(at, 1) == group * pair_rows + iota(at, 0) // aminos
    col_pick = iota(at, 1) == rank * aminos + iota(at, 0) % aminos
    both = jnp.zeros((pairs, LANES), F32)
    take(far.at[:, :, high], flag_r)
    for seen in (near_aux[:, LANES:], flat(far[:, :, LANES:])):
        both = both + dot(one_hot(row_pick), seen) * dot(one_hot(col_pick), seen)
    counts = jnp.sum(both, axis=1, keepdims=True)
    resolved = jnp.broadcast_to(resolved_ref[...].astype(F32), at)
    scale = jnp.sum(jnp.where(row_pick, resolved, 0.0), axis=1, keepdims=True) * jnp.sum(
        jnp.where(col_pick, resolved, 0.0), axis=1, keepdims=True) / counts
    scale = jnp.broadcast_to(scale, (pairs, LANES))
    take(outer_ref, load_s.at[5])
    take(side_all, side_r)
    right_rows = flat(side_buf[quads])
    products = [dot(flat(side_buf[q]), right_rows, 0, 0) for q in range(quads)]
    parts = []
    step = folds * aminos
    for c in range(0, PROJ_FEATURES // folds, aminos):
        slabs = []
        for x in range(c, c + aminos):
            slab = [product[x * step:(x + 1) * step] for product in products]
            slabs.append(jnp.concatenate(slab, axis=0).astype(BF16))
        parts.append(jnp.concatenate(turn_blocks(slabs), axis=0))
    outer = dot(jnp.concatenate(parts, axis=1), outer_ref[...].reshape(-1, folds * CZ))
    for j in range(aminos):
        for q in range(quads):
            base = (j * quads + q) * folds * aminos
            total = outer[base:base + aminos, :CZ]
            for x in range(1, folds):
                row = base + x * aminos
                total = total + outer[row:row + aminos, x * CZ:(x + 1) * CZ]
            turn_buf[pl.ds(q * aminos * aminos + j, aminos, stride=aminos), :] = total
    result = pair_value + scale * turn_buf[...]
    pair_out_ref[...] = result.reshape(pair_rows, aminos, CZ).astype(BF16)
    take(out_all, out_r)
    for view in (near_all, far, side_all, out_all):
        take(view, send_s)


def write_kernel(out_ref, pair_ref, out_hbm, pair_hbm, sem):
    copies = [pltpu.make_async_copy(out_ref, out_hbm, sem.at[0]),
              pltpu.make_async_copy(pair_ref, pair_hbm, sem.at[1])]
    for copy in copies:
        copy.start()
    for copy in copies:
        copy.wait()


def fused(*args):
    emb, mask, resolved, pair = args[:4]
    groups, ranks = lax.axis_size("seq"), lax.axis_size("res")
    chains, aminos = emb.shape[:2]
    per = chains // ranks
    pair_rows = pair.shape[0]
    quads = pair_rows // aminos
    devices = groups * ranks
    folds = 8 // aminos
    operands = (emb.reshape(ranks, per, aminos, ROW_FEATURES), mask.T, resolved.reshape(1, -1), pair, args[4], args[5].T, args[6],
                args[7].T, args[8].reshape(PROJ_FEATURES // folds, folds, PROJ_FEATURES, CZ))
    vmem = pl.BlockSpec(memory_space=pltpu.VMEM)
    whole = pl.BlockSpec(memory_space=pl.ANY)
    dma = pltpu.SemaphoreType.DMA
    results = pl.pallas_call(
        functools.partial(fused_kernel, groups, ranks, per, aminos),
        out_shape=(pltpu.VMEM(emb.shape, BF16), pltpu.VMEM(pair.shape, BF16)),
        in_specs=[whole] * len(operands),
        out_specs=(vmem, vmem),
        scratch_shapes=[
            pltpu.VMEM((ranks, per + 1, aminos, ROW_FEATURES), BF16),
            pltpu.VMEM((per + 1, ranks, aminos, ROW_FEATURES), BF16),
            pltpu.VMEM((ranks, aminos, ROW_FEATURES), BF16),
        ] + [pltpu.VMEM(x.shape, x.dtype) for x in operands[1:8]] + [
            pltpu.VMEM((PROJ_FEATURES // folds, PROJ_FEATURES, folds * CZ), BF16),
            pltpu.VMEM((groups, ranks, quads + 1, per, LANES), BF16),
            pltpu.VMEM((quads + 1, devices, per, LANES), BF16),
            pltpu.VMEM((per, ranks, aminos, ROW_FEATURES), BF16),
            pltpu.VMEM((chains * aminos, ROW_FEATURES), F32),
            pltpu.VMEM((chains * aminos, LANES), F32),
            pltpu.VMEM((chains * aminos, 2 * LANES), F32),
            pltpu.VMEM((chains * aminos, ROW_FEATURES), F32),
            pltpu.VMEM((chains * aminos, ROW_FEATURES), BF16),
            pltpu.VMEM((LANES, per * LANES), BF16),
            pltpu.VMEM((chains, chains * aminos), BF16),
            pltpu.VMEM((2 * LANES, ROW_FEATURES), BF16),
            pltpu.VMEM((pair_rows * aminos, CZ), F32),
            dma((6,)), dma, dma, dma, dma, dma, dma,
        ],
        compiler_params=pltpu.CompilerParams(collective_id=0, has_side_effects=True),
    )(*operands)
    return pl.pallas_call(
        write_kernel,
        out_shape=(jax.ShapeDtypeStruct(emb.shape, BF16), jax.ShapeDtypeStruct(pair.shape, BF16)),
        in_specs=[whole, whole],
        out_specs=(whole, whole),
        scratch_shapes=[dma((2,))],
    )(*[pltpu.with_memory_space_constraint(x, pltpu.VMEM) for x in results])


def fits(mesh, emb, pair):
    groups, ranks = mesh.shape["seq"], mesh.shape["res"]
    chains, aminos = emb.shape[:2]
    if chains % ranks or aminos * PROJ_FEATURES != LANES or chains * aminos != LANES:
        return False
    if ranks & (ranks - 1) or HEAD_NUMBER * PER_HEAD_DIM != groups * LANES:
        return False
    pairs = pair.shape[0] * aminos
    return pairs * groups == LANES and chains // ranks * aminos * groups == PROJ_FEATURES


def solution(mesh):
    placed = (
        P(("crop", "seq"), "res", None),
        P(("crop", "seq"), "res"),
        P("crop"),
        P(("crop", "seq"), "res", None),
        P(),
        P(),
        P(),
        P(),
        P(),
    )
    def either(*args):
        return (fused if fits(mesh, args[0], args[3]) else per_device)(*args)

    return jax.shard_map(
        either,
        mesh=mesh,
        in_specs=placed,
        out_specs=(P(("crop", "seq"), "res", None), P(("crop", "seq"), "res", None)),
        check_vma=False,
    )
```
